32 devices in a mesh: data: 1 (over z), col: 4 (over y), row: 8 (over x, core).
Axes of the slice: x: 4, y: 4, z: 1, core: 2. Of those that a mesh axis runs over, the one named last changes fastest.
The devices are a block of a 4x4x8 slice.
Arguments:
- x: bfloat16 [24, 6, 4096], P(None, 'data', 'row')
- w_x1: bfloat16 [2, 4096, 16384], P(None, 'row', 'col')
- w_h1: bfloat16 [2, 4096, 16384], P(None, 'row', 'col')
- b_1: float32 [2, 16384], P(None, 'col')
- w_x2: bfloat16 [2, 4096, 16384], P(None, 'row', 'col')
- w_h2: bfloat16 [4096, 16384], P('row', 'col')
- b_2: float32 [16384], P('col')
- h_zero: float32 [3, 6, 4096], P(None, 'data', 'row')
- c_zero: float32 [3, 6, 4096], P(None, 'data', 'row')
Outputs:
- output 1: bfloat16 [24, 6, 4096], P(None, 'data', ('col', 'row'))
- output 2: float32 [3, 6, 4096], P(None, 'data', ('col', 'row'))
All inputs are finite; a program needn't handle non-finite values.
Results may differ from the reference program's by a relative error of at most 0.00336537.
Values are sent between devices in bfloat16 or wider.
A program may use at most 768 MiB of HBM per device.

```python
import jax
import jax.numpy as jnp
from jax import lax

STEPS = 24
BATCH = 6
D = 4096


def setup_inputs(seed: int = 0, part: int = 0) -> dict:
    key = jax.random.key(seed)
    shared = jax.random.split(key, 6)
    own = jax.random.split(jax.random.fold_in(key, part), 3)
    in_scale = D ** -0.5
    x = jax.random.normal(own[0], (STEPS, BATCH, D), jnp.float32)
    w_x1 = jax.random.normal(shared[0], (2, D, 4 * D), jnp.float32) * in_scale
    w_h1 = jax.random.normal(shared[1], (2, D, 4 * D), jnp.float32) * in_scale
    b_1 = 0.5 * jax.random.normal(shared[2], (2, 4 * D), jnp.float32)
    w_x2 = jax.random.normal(shared[3], (2, D, 4 * D), jnp.float32) * in_scale
    w_h2 = jax.random.normal(shared[4], (D, 4 * D), jnp.float32) * in_scale
    b_2 = 0.5 * jax.random.normal(shared[5], (4 * D,), jnp.float32)
    h_zero = 0.9 * jnp.tanh(jax.random.normal(own[1], (3, BATCH, D), jnp.float32))
    c_zero = 1.5 * jax.random.normal(own[2], (3, BATCH, D), jnp.float32)
    return {'x': x.astype(jnp.bfloat16), 'w_x1': w_x1.astype(jnp.bfloat16),
            'w_h1': w_h1.astype(jnp.bfloat16), 'b_1': b_1,
            'w_x2': w_x2.astype(jnp.bfloat16), 'w_h2': w_h2.astype(jnp.bfloat16),
            'b_2': b_2, 'h_zero': h_zero, 'c_zero': c_zero}


def lstm_layer(in_seq, w_in, w_rec, gate_bias, h_init, c_init, backward):
    def one_step(carry, in_t):
        h_prev, c_prev = carry
        z_all = (jnp.dot(in_t, w_in, preferred_element_type=jnp.float32)
                 + jnp.dot(h_prev, w_rec, preferred_element_type=jnp.float32) + gate_bias)
        gates = z_all.reshape(z_all.shape[0], D, 4)
        c_next = (jax.nn.sigmoid(gates[:, :, 1]) * c_prev
                  + jax.nn.sigmoid(gates[:, :, 0]) * jnp.tanh(gates[:, :, 2]))
        h_next = (jax.nn.sigmoid(gates[:, :, 3]) * jnp.tanh(c_next)).astype(jnp.bfloat16)
        return (h_next, c_next), h_next
    carry_out, h_seq = lax.scan(one_step, (h_init.astype(jnp.bfloat16), c_init), in_seq, reverse=backward)
    return h_seq, carry_out[1]


def reference(x, w_x1, w_h1, b_1, w_x2, w_h2, b_2, h_zero, c_zero):
    fwd_seq, fwd_cell = lstm_layer(x, w_x1[0], w_h1[0], b_1[0], h_zero[0], c_zero[0], False)
    bwd_seq, bwd_cell = lstm_layer(x, w_x1[1], w_h1[1], b_1[1], h_zero[1], c_zero[1], True)
    mid_seq = jnp.concatenate([fwd_seq, bwd_seq], axis=2)
    top_seq, top_cell = lstm_layer(mid_seq, w_x2.reshape(2 * D, 4 * D), w_h2, b_2,
                                   h_zero[2], c_zero[2], False)
    return top_seq, jnp.stack([fwd_cell, bwd_cell, top_cell])
```

```python
import functools

import jax
import jax.numpy as jnp
from jax import lax
from jax.experimental import pallas as pl
from jax.experimental.pallas import tpu as pltpu
from jax.sharding import PartitionSpec as P

PAD = 8
STAGES = 4
SPAN = 8
F32, BF16 = jnp.float32, jnp.bfloat16


def nbytes_wait(ref, sem):
    pltpu.make_async_copy(ref, ref, sem).wait()


def hop_groups(n_x, n_y):
    far = {}
    for dy in range(n_y):
        for dx in range(n_x):
            far.setdefault(min(dx, n_x - dx) + min(dy, n_y - dy), []).append((dx, dy))
    return [far[k] for k in sorted(far)]


def kernel(n_row, n_col, x_ref, h0_ref, c0_ref, b1_ref, b2_ref, w_x1, w_h1, w_x2, w_h2, out_h, out_c,
           w_one, w_two, w_mid, send_a, send_b, send_c, stage, sort, part_own, part_oth, part_in, xz_in,
           mid_in, z_in, lhs, hs1, hs2, h_oth, c_all1, c_all2, c_st, ho, co,
           stage_sem, wsend_sem, w_sem, pair_send, pair_sem, xz_send, xz_sem, mid_send, mid_sem, z_send, z_sem,
           init_send, h0_sem, c0_sem, step_send, step_sem, fwd_send, fwd_sem, end_send, end_sem):
    n_x = n_row // 2
    n_step = x_ref.shape[0] // PAD
    n_span = n_step // SPAN
    deep = w_h2.shape[0]
    wide = w_h2.shape[1] // n_row
    unit = wide // 4
    half_k = deep // 2
    r = lax.axis_index('row')
    y = lax.axis_index('col')
    core = lax.rem(r, 2)
    x = lax.div(r, 2)
    mate = r + 1 - 2 * core
    own_j = y * n_x + x

    def at(row, col):
        return {'row': row, 'col': col}

    def remote(src, dst, ssem, rsem, row, col):
        return pltpu.make_async_remote_copy(src_ref=src, dst_ref=dst, send_sem=ssem, recv_sem=rsem,
                                            device_id=at(row, col), device_id_type=pl.DeviceIdType.MESH)

    barrier = pltpu.get_barrier_semaphore()
    for dc in range(n_col):
        for dr in range(n_row):
            if dc or dr:
                pl.semaphore_signal(barrier, inc=1, device_id=at(lax.rem(r + dr, n_row), lax.rem(y + dc, n_col)),
                                    device_id_type=pl.DeviceIdType.MESH)
    pl.semaphore_wait(barrier, n_col * n_row - 1)

    first = core * n_step
    for d in range(1, n_row):
        to = lax.rem(r + d, n_row)
        tc = lax.rem(to, 2)
        here = pl.ds(2 * r, 2)
        remote(h0_ref.at[tc], hs1.at[tc * n_step, here], init_send, h0_sem.at[0], to, y).start()
        remote(h0_ref.at[2], hs2.at[0, here], init_send, h0_sem.at[1], to, y).start()
        remote(c0_ref.at[tc], c_all1.at[here], init_send, c0_sem.at[0], to, y).start()
        remote(c0_ref.at[2], c_all2.at[here], init_send, c0_sem.at[1], to, y).start()
    hs1[first, pl.ds(2 * r, 2)] = h0_ref[core]
    hs2[0, pl.ds(2 * r, 2)] = h0_ref[2]
    c_all1[pl.ds(2 * r, 2)] = c0_ref[core]
    c_all2[pl.ds(2 * r, 2)] = c0_ref[2]

    rows_i = lax.broadcasted_iota(jnp.int32, (wide, wide), 0)
    cols_i = lax.broadcasted_iota(jnp.int32, (wide, wide), 1)
    gate_i, unit_i = lax.div(cols_i, unit), lax.rem(cols_i, unit)
    sort[...] = jnp.where(rows_i == 4 * unit_i + gate_i, 1.0, 0.0).astype(BF16)

    def group_of(i):
        k = lax.div(i, 2)
        dx = lax.rem(2 + lax.div(k, 2) * 3 + lax.rem(k, 2) * (n_x - 3 + lax.div(k, 2) * 2), n_x)
        return 2 * lax.rem(x + dx, n_x) + lax.rem(i, 2)

    def load(src, i, slot):
        g = group_of(i)
        return pltpu.make_async_copy(src.at[:, pl.ds(pl.multiple_of(g * wide, wide), wide)], stage.at[slot],
                                     stage_sem.at[slot])

    def send_weights(buf, dst, tgt_core, wi):
        def use(g, tile):
            buf[g] = tile
            tx, half = lax.div(g, 2), lax.rem(g, 2)
            to = 2 * tx + tgt_core

            @pl.when(to == r)
            def _():
                dst[r, half] = tile

            @pl.when(to != r)
            def _():
                remote(buf.at[g], dst.at[r, half], wsend_sem, w_sem.at[wi], to, y).start()
        return use

    def project(k):
        def use(g, tile):
            z = jnp.dot(x_ref[...], tile, preferred_element_type=F32)

            @pl.when(core == k)
            def _():
                for q in range(n_span):
                    part_own[q, g] = z[q * SPAN * PAD:(q + 1) * SPAN * PAD]

            @pl.when(core != k)
            def _():
                for q in range(n_span):
                    part_oth[q, g] = z[q * SPAN * PAD:(q + 1) * SPAN * PAD]
        return use

    def keep(k):
        def use(g, tile):
            w_mid[k, g] = tile
        return use

    jobs = [(w_h1.at[1], send_weights(send_a, w_one, 1, 0)), (w_h1.at[0], send_weights(send_b, w_one, 0, 0)),
            (w_x1.at[1], project(1)), (w_x1.at[0], project(0)),
            (w_h2, send_weights(send_c, w_two, 1, 1)), (w_x2.at[0], keep(0)), (w_x2.at[1], keep(1))]
    for i in range(STAGES - 1):
        load(jobs[0][0], i, i).start()

    def partner_sum():
        for q in range(n_span):
            remote(part_oth.at[q], part_in.at[q], pair_send, pair_sem.at[q], mate, y).start()
        for i in range(n_span):
            q_s = i + core * (n_span - 1 - 2 * i)
            nbytes_wait(part_in.at[q_s], pair_sem.at[q_s])

            def add(g, c):
                part_own[q_s, g] += part_in[q_s, g]
                return c
            lax.fori_loop(0, n_row, add, 0)
            for d in range(1, n_x):
                tx = lax.rem(x + d, n_x)
                remote(part_own.at[q_s, pl.ds(2 * tx, 2)], xz_in.at[q_s, n_x - 1 - d], xz_send, xz_sem.at[q_s],
                       2 * tx + core, y).start()

    for n, (src, use) in enumerate(jobs):
        following = jobs[n + 1][0] if n + 1 < len(jobs) else None

        def body(i, c):
            slot = lax.rem(i, STAGES)
            load(src, i, slot).wait()
            ahead = i + STAGES - 1
            slot_ahead = lax.rem(ahead, STAGES)

            @pl.when(ahead < n_row)
            def _():
                load(src, ahead, slot_ahead).start()
            if following is not None:
                @pl.when(ahead >= n_row)
                def _():
                    load(following, ahead - n_row, slot_ahead).start()
            tile = jnp.dot(stage[slot], sort[...], preferred_element_type=F32).astype(BF16)
            use(group_of(i), tile)
            return c
        lax.fori_loop(0, n_row, body, 0)
        if n == 3:
            partner_sum()

    groups = hop_groups(n_x, n_col)
    offsets = [o for grp in groups for o in grp]
    index = {o: i for i, o in enumerate(offsets)}

    def receive(hs, slot, dx, dy, parity):
        j = lax.rem(y + dy, n_col) * n_x + lax.rem(x + dx, n_x)
        nbytes_wait(hs.at[slot, j], step_sem.at[parity, index[dx, dy]])

    def chain_step(hs, w, prev, new, s, z_of, b_ref, last_send, after_receive):
        parity = lax.rem(s, 2)
        acc = [z_of(hf) + b_ref[2 * x + hf] for hf in range(2)]
        for n, grp in enumerate(groups):
            if n:
                @pl.when(s > 0)
                def _():
                    for dx, dy in grp:
                        receive(hs, prev, dx, dy, 1 - parity)
            if n == len(groups) - 1 and after_receive is not None:
                after_receive()
            for dx, dy in grp:
                sx, sy = lax.rem(x + dx, n_x), lax.rem(y + dy, n_col)
                j = sy * n_x + sx
                h = hs[prev, j]
                rows = pl.ds(pl.multiple_of(lax.rem(j, 2) * half_k, half_k), half_k)
                for hf in range(2):
                    acc[hf] += jnp.dot(h, w[lax.div(j, 2), hf, rows], preferred_element_type=F32)
        h_new = []
        for hf in range(2):
            gate = [acc[hf][:, k * unit:(k + 1) * unit] for k in range(4)]
            c = (jax.nn.sigmoid(gate[1]) * c_st[hf]
                 + jax.nn.sigmoid(gate[0]) * jnp.tanh(gate[2]))
            c_st[hf] = c
            h = (jax.nn.sigmoid(gate[3]) * jnp.tanh(c)).astype(BF16)
            hs[new, own_j, :, hf * unit:(hf + 1) * unit] = h
            h_new.append(h)

        def send():
            for dx, dy in reversed(offsets[1:]):
                remote(hs.at[new, own_j], hs.at[new, own_j], step_send,
                       step_sem.at[parity, index[(n_x - dx) % n_x, (n_col - dy) % n_col]],
                       2 * lax.rem(x + dx, n_x) + core, lax.rem(y + dy, n_col)).start()
        if last_send:
            send()
        else:
            pl.when(s < n_step - 1)(send)
        return h_new

    def own_state(c_all):
        for hf in range(2):
            c_st[hf] = c_all[own_j, :, hf * unit:(hf + 1) * unit]

    nbytes_wait(hs1.at[0, pl.ds(0, 2 * n_row - 2)], h0_sem.at[0])
    nbytes_wait(hs2.at[0, pl.ds(0, 2 * n_row - 2)], h0_sem.at[1])
    nbytes_wait(c_all1.at[pl.ds(0, 2 * n_row - 2)], c0_sem.at[0])
    nbytes_wait(c_all2.at[pl.ds(0, 2 * n_row - 2)], c0_sem.at[1])
    own_state(c_all1)
    nbytes_wait(w_one.at[pl.ds(0, n_row - 1)], w_sem.at[0])

    def to_mate(slot):
        time = slot - 1 + core
        return remote(hs1.at[slot, pl.ds(2 * mate, 2)], h_oth.at[time], fwd_send, fwd_sem, mate, y)

    def step_one(s, c):
        t = s + core * (n_step - 1 - 2 * s)
        q = lax.div(t, SPAN)
        at_row = pl.ds(pl.multiple_of(lax.rem(t, SPAN) * PAD, PAD), PAD)

        @pl.when(lax.rem(s, SPAN) == 0)
        def _():
            nbytes_wait(xz_in.at[q], xz_sem.at[q])

        def z_of(hf):
            z = part_own[q, 2 * x + hf, at_row]
            for d in range(n_x - 1):
                z = z + xz_in[q, d, hf, at_row]
            return z

        def pass_on():
            @pl.when(s > 0)
            def _():
                to_mate(t + core).start()
        chain_step(hs1, w_one, t + core, t + 1 - core, s, z_of, b1_ref.at[core], True, pass_on)
        return c
    lax.fori_loop(0, n_step, step_one, 0)
    end_slot = n_step - n_step * core
    for n, grp in enumerate(groups):
        if n:
            for dx, dy in grp:
                receive(hs1, end_slot, dx, dy, (n_step - 1) % 2)
    to_mate(end_slot).start()
    for hf in range(2):
        c_end = c_st[hf]

        @pl.when(core == hf)
        def _():
            out_c[core] = c_end

        @pl.when(core != hf)
        def _():
            co[core] = c_end

    nbytes_wait(h_oth, fwd_sem)
    nbytes_wait(part_oth, pair_send)

    def mid_span(q, c):
        for i in range(SPAN):
            for jj in range(2):
                here = slice(i * PAD, (i + 1) * PAD), slice(jj * half_k, (jj + 1) * half_k)
                lhs[0, here[0], here[1]] = hs1[q * SPAN + i + 1 - core, 2 * r + jj].astype(F32)
                lhs[1, here[0], here[1]] = h_oth[q * SPAN + i, jj].astype(F32)
        left, right = lhs[0].astype(BF16), lhs[1].astype(BF16)

        def one(g, c):
            part_oth[q, g] = (jnp.dot(left, w_mid[core, g], preferred_element_type=F32)
                              + jnp.dot(right, w_mid[1 - core, g], preferred_element_type=F32))
            return c
        lax.fori_loop(0, n_row, one, 0)

        @pl.when(core == 1)
        def _():
            remote(part_oth.at[q], mid_in.at[q], mid_send, mid_sem.at[q], mate, y).start()

        @pl.when(core == 0)
        def _():
            nbytes_wait(mid_in.at[q], mid_sem.at[q])

            def add(g, c):
                part_oth[q, g] += mid_in[q, g]
                return c
            lax.fori_loop(0, n_row, add, 0)
            for d in range(n_x):
                tx = lax.rem(x + d, n_x)
                remote(part_oth.at[q, pl.ds(2 * tx, 2)], z_in.at[q, (n_x - d) % n_x], z_send, z_sem.at[q],
                       2 * tx + 1, y).start()
        return c
    lax.fori_loop(0, n_span, mid_span, 0)

    @pl.when(core == 1)
    def _():
        own_state(c_all2)
        nbytes_wait(w_two.at[pl.ds(0, n_row - 1)], w_sem.at[1])

        def step_two(t, c):
            q = lax.div(t, SPAN)
            at_row = pl.ds(pl.multiple_of(lax.rem(t, SPAN) * PAD, PAD), PAD)

            @pl.when(lax.rem(t, SPAN) == 0)
            def _():
                nbytes_wait(z_in.at[q], z_sem.at[q])

            def z_of(hf):
                z = z_in[q, 0, hf, at_row]
                for d in range(1, n_x):
                    z = z + z_in[q, d, hf, at_row]
                return z
            h_new = chain_step(hs2, w_two, t, t + 1, t, z_of, b2_ref, False, None)
            ho[t] = h_new[0]
            out_h[t] = h_new[1]
            return c
        lax.fori_loop(0, n_step, step_two, 0)
        co[2] = c_st[0]
        out_c[2] = c_st[1]
        ends = [remote(ho, out_h, end_send.at[0], end_sem.at[0], mate, y),
                remote(co.at[pl.ds(1, 2)], out_c.at[pl.ds(1, 2)], end_send.at[1], end_sem.at[1], mate, y)]
        for e in ends:
            e.start()
        for e in ends:
            e.wait_send()
        nbytes_wait(out_c.at[0], end_sem.at[2])
        nbytes_wait(hs2.at[pl.ds(0, n_step - 1), pl.ds(0, n_x * n_col - 1)], step_send)
        nbytes_wait(part_oth, mid_send)
        nbytes_wait(send_c.at[pl.ds(0, n_row - 4)], wsend_sem)

    @pl.when(core == 0)
    def _():
        e = remote(co.at[0], out_c.at[0], end_send.at[2], end_sem.at[2], mate, y)
        e.start()
        e.wait_send()
        nbytes_wait(out_h, end_sem.at[0])
        nbytes_wait(out_c.at[pl.ds(1, 2)], end_sem.at[1])
        nbytes_wait(part_oth, z_send)
        nbytes_wait(send_c.at[pl.ds(0, n_row - 2)], wsend_sem)

    nbytes_wait(hs1.at[pl.ds(0, n_step), pl.ds(0, n_x * n_col - 1)], step_send)
    nbytes_wait(h_oth, fwd_send)
    nbytes_wait(xz_in, xz_send)
    nbytes_wait(hs1.at[0, pl.ds(0, 2 * n_row - 2)], init_send)
    nbytes_wait(hs1.at[0, pl.ds(0, 2 * n_row - 2)], init_send)
    nbytes_wait(c_all1.at[pl.ds(0, 2 * n_row - 2)], init_send)
    nbytes_wait(c_all1.at[pl.ds(0, 2 * n_row - 2)], init_send)
    nbytes_wait(send_a, wsend_sem)
    nbytes_wait(send_b, wsend_sem)


def solution(mesh):
    n_row = mesh.shape['row']
    n_col = mesh.shape['col']
    spec_seq = P(None, 'data', 'row')
    spec_weight = P(None, 'row', 'col')
    spec_out = P(None, 'data', ('col', 'row'))

    def local(x_rows, w_x1, w_h1, b_1, w_x2, w_h2, b_2, h_zero, c_zero):
        n_step, batch, deep = x_rows.shape
        cols = w_h2.shape[1]
        wide = cols // n_row
        unit = wide // 4
        n_chunk = n_row // 2 * n_col
        chunk = 2 * unit
        n_span = n_step // SPAN

        def padded(v):
            return jnp.pad(v, ((0, 0), (0, PAD - batch), (0, 0)))

        def by_chunk(v):
            return padded(v).reshape(3, PAD, 2, chunk).transpose(0, 2, 1, 3)

        x_in = padded(x_rows).reshape(n_step * PAD, deep)
        h_in = by_chunk(h_zero.astype(BF16))
        c_in = by_chunk(c_zero)
        bias1 = b_1.reshape(2, n_row, unit, 4).transpose(0, 1, 3, 2).reshape(2, n_row, 1, wide)
        bias2 = b_2.reshape(n_row, unit, 4).transpose(0, 2, 1).reshape(n_row, 1, wide)
        vmem = pl.BlockSpec(memory_space=pltpu.VMEM)
        hbm = pl.BlockSpec(memory_space=pl.ANY)
        dma = pltpu.SemaphoreType.DMA
        rows = SPAN * PAD
        weights = (n_row, 2, deep, wide)
        h_out, c_out = pl.pallas_call(
            functools.partial(kernel, n_row, n_col),
            out_shape=(jax.ShapeDtypeStruct((n_step, PAD, unit), BF16),
                       jax.ShapeDtypeStruct((3, PAD, unit), F32)),
            in_specs=[vmem] * 5 + [hbm] * 4,
            out_specs=(vmem, vmem),
            scratch_shapes=[
                pltpu.VMEM(weights, BF16),
                pltpu.VMEM(weights, BF16),
                pltpu.VMEM((2, n_row, deep, wide), BF16),
                pltpu.VMEM((n_row, deep, wide), BF16),
                pltpu.VMEM((n_row, deep, wide), BF16),
                pltpu.VMEM((n_row, deep, wide), BF16),
                pltpu.VMEM((STAGES, deep, wide), BF16),
                pltpu.VMEM((wide, wide), BF16),
                pltpu.VMEM((n_span, n_row, rows, wide), F32),
                pltpu.VMEM((n_span, n_row, rows, wide), F32),
                pltpu.VMEM((n_span, n_row, rows, wide), F32),
                pltpu.VMEM((n_span, n_row // 2 - 1, 2, rows, wide), F32),
                pltpu.VMEM((n_span, n_row, rows, wide), F32),
                pltpu.VMEM((n_span, n_row // 2, 2, rows, wide), F32),
                pltpu.VMEM((2, rows, deep), F32),
                pltpu.VMEM((n_step + 1, n_chunk, PAD, chunk), BF16),
                pltpu.VMEM((n_step + 1, n_chunk, PAD, chunk), BF16),
                pltpu.VMEM((n_step, 2, PAD, chunk), BF16),
                pltpu.VMEM((n_chunk, PAD, chunk), F32),
                pltpu.VMEM((n_chunk, PAD, chunk), F32),
                pltpu.VMEM((2, PAD, unit), F32),
                pltpu.VMEM((n_step, PAD, unit), BF16),
                pltpu.VMEM((3, PAD, unit), F32),
                dma((STAGES,)), dma(()), dma((2,)),
                dma(()), dma((n_span,)),
                dma(()), dma((n_span,)),
                dma(()), dma((n_span,)),
                dma(()), dma((n_span,)),
                dma(()), dma((2,)), dma((2,)),
                dma(()), dma((2, n_chunk)),
                dma(()), dma(()),
                dma((3,)), dma((3,)),
            ],
            compiler_params=pltpu.CompilerParams(collective_id=0, has_side_effects=True,
                                                 vmem_limit_bytes=67_043_328),
        )(x_in, h_in, c_in, bias1, bias2, w_x1, w_h1, w_x2, w_h2)
        return h_out[:, :batch], c_out[:, :batch]

    return jax.shard_map(local, mesh=mesh,
                         in_specs=(spec_seq, spec_weight, spec_weight, P(None, 'col'), spec_weight,
                                   P('row', 'col'), P('col'), spec_seq, spec_seq),
                         out_specs=(spec_out, spec_out), check_vma=False)
```

```python
import functools

import jax
import jax.numpy as jnp
from jax import lax
from jax.experimental import pallas as pl
from jax.experimental.pallas import tpu as pltpu
from jax.sharding import PartitionSpec as P

PAD = 8
STAGES = 4
BATCH = 2
PIECES = 8
F32, BF16 = jnp.float32, jnp.bfloat16


def nbytes_wait(ref, sem):
    pltpu.make_async_copy(ref, ref, sem).wait()


def hop_groups(n_x, n_y):
    far = {}
    for dy in range(n_y):
        for dx in range(n_x):
            far.setdefault(min(dx, n_x - dx) + min(dy, n_y - dy), []).append((dx, dy))
    return [far[k] for k in sorted(far)]


def kernel(n_row, n_col, x_ref, h0_ref, c0_ref, b1_ref, b2_ref, w_x1, w_h1, w_x2, w_h2, out_h, out_c,
           w_one, w_two, w_fwd, w_mid, send_a, send_c, stage, sort, p_b, p_f, xz_in, z_in, z_out, z_part, lhs,
           hs1, hs2, h_oth, c_all1, c_all2, c_st, ho, co,
           stage_sem, a_send, w_sem, f_send, f_sem, c_send, pf_send, pf_sem, pb_send, pb_sem, xz_send, xz_sem,
           mid_send, z_sem, init_send, h0_sem, c0_sem, step_send, step_sem, part_send, part_sem, row_sem,
           fwd_send, fwd_sem, end_send, end_sem):
    n_x = n_row // 2
    n_step = x_ref.shape[0] // PAD
    n_bat = n_step // BATCH
    deep = w_h2.shape[0]
    wide = w_h2.shape[1] // n_row
    unit = wide // 4
    chunk = deep // 2
    r = lax.axis_index('row')
    y = lax.axis_index('col')
    core = lax.rem(r, 2)
    x = lax.div(r, 2)
    mate = r + 1 - 2 * core
    own_j = y * n_x + x

    def at(row, col):
        return {'row': row, 'col': col}

    def remote(src, dst, ssem, rsem, row, col):
        return pltpu.make_async_remote_copy(src_ref=src, dst_ref=dst, send_sem=ssem, recv_sem=rsem,
                                            device_id=at(row, col), device_id_type=pl.DeviceIdType.MESH)

    def group_of(i):
        dx = jnp.where(i < 4, 1 + 2 * lax.rem(i, 2), 2 - 2 * lax.div(i - 4, 2))
        half = jnp.where(i < 4, lax.div(i, 2), lax.rem(i, 2))
        return lax.rem(x + dx, n_x), half

    def load(src, i, slot):
        tx, half = group_of(i)
        first = pl.multiple_of((2 * tx + half) * wide, wide)
        pltpu.make_async_copy(src.at[:, pl.ds(first, wide)], stage.at[slot], stage_sem.at[slot]).start()

    def load_late(n):
        slot, i = lax.rem(n, STAGES), lax.rem(n, n_row)

        @pl.when(n < n_row)
        def _():
            load(w_h2, i, slot)

        @pl.when(jnp.logical_and(n >= n_row, n < 3 * n_row))
        def _():
            load(w_x2.at[lax.div(n - n_row, n_row)], i, slot)

    def sorted_tile(slot):
        return jnp.dot(stage[slot], sort[...], preferred_element_type=F32).astype(BF16)

    def use_back(tx, half, tile):
        @pl.when(jnp.logical_and(tx == x, core == 1))
        def _():
            w_one[r, half] = tile

        @pl.when(jnp.logical_or(tx != x, core == 0))
        def _():
            g = 2 * tx + half
            send_a[g] = tile
            remote(send_a.at[g], w_one.at[r, half], a_send, w_sem.at[0], 2 * tx + 1, y).start()

    def use_fwd(tx, half, tile):
        g = 2 * tx + half
        w_fwd[0, g] = tile

        @pl.when(core == 1)
        def _():
            remote(w_fwd.at[0, g], w_fwd.at[1, g], f_send, f_sem, mate, y).start()

    def project(buf):
        def use(tx, half, tile):
            z = jnp.dot(x_ref[...], tile, preferred_element_type=F32)
            for m in range(n_bat):
                buf[m, tx, half] = z[m * BATCH * PAD:(m + 1) * BATCH * PAD]
        return use

    def late_tile(n):
        slot = lax.rem(n, STAGES)
        nbytes_wait(stage.at[slot], stage_sem.at[slot])
        load_late(n + STAGES - 1)
        tile = sorted_tile(slot)
        tx, half = group_of(lax.rem(n, n_row))
        g = 2 * tx + half

        @pl.when(n >= n_row)
        def _():
            w_mid[lax.div(n - n_row, n_row), g] = tile

        @pl.when(jnp.logical_and(n < n_row, jnp.logical_and(tx == x, core == 1)))
        def _():
            w_two[r, half] = tile

        @pl.when(jnp.logical_and(n < n_row, jnp.logical_or(tx != x, core == 0)))
        def _():
            send_c[g] = tile

        @pl.when(jnp.logical_and(n < n_row, jnp.logical_and(tx == x, core == 0)))
        def _():
            remote(send_c.at[g], w_two.at[r, half], c_send, w_sem.at[1], mate, y).start()

    def piece(p):
        k, e = lax.div(p, 2), lax.rem(p, 2)
        near = k < 2 * PIECES
        tx = lax.rem(x + jnp.where(near, 1 + 2 * e, 2), n_x)
        half = jnp.where(near, lax.div(k, PIECES), e)
        n_rows = deep // PIECES
        rows = pl.ds(pl.multiple_of(lax.rem(k, PIECES) * n_rows, n_rows), n_rows)
        remote(send_c.at[2 * tx + half, rows], w_two.at[r, half, rows], c_send, w_sem.at[1], 2 * tx + 1, y).start()

    jobs = [(w_h1.at[1], use_back), (w_h1.at[0], use_fwd), (w_x1.at[0], project(p_f)), (w_x1.at[1], project(p_b))]
    for i in range(STAGES - 1):
        load(jobs[0][0], i, i)

    rows_i = lax.broadcasted_iota(jnp.int32, (wide, wide), 0)
    cols_i = lax.broadcasted_iota(jnp.int32, (wide, wide), 1)
    gate_i, unit_i = lax.div(cols_i, unit), lax.rem(cols_i, unit)
    sort[...] = jnp.where(rows_i == 4 * unit_i + gate_i, 1.0, 0.0).astype(BF16)

    barrier = pltpu.get_barrier_semaphore()
    for dc in range(n_col):
        for dr in range(n_row):
            if dc or dr:
                pl.semaphore_signal(barrier, inc=1, device_id=at(lax.rem(r + dr, n_row), lax.rem(y + dc, n_col)),
                                    device_id_type=pl.DeviceIdType.MESH)
    pl.semaphore_wait(barrier, n_col * n_row - 1)

    for d in range(1, n_row):
        to = lax.rem(r + d, n_row)
        tc = lax.rem(to, 2)
        here = pl.ds(2 * r, 2)
        remote(h0_ref.at[tc], hs1.at[tc * n_step, here], init_send, h0_sem.at[0], to, y).start()
        remote(h0_ref.at[2], hs2.at[0, here], init_send, h0_sem.at[1], to, y).start()
        remote(c0_ref.at[tc], c_all1.at[here], init_send, c0_sem.at[0], to, y).start()
        remote(c0_ref.at[2], c_all2.at[here], init_send, c0_sem.at[1], to, y).start()
    hs1[core * n_step, pl.ds(2 * r, 2)] = h0_ref[core]
    hs2[0, pl.ds(2 * r, 2)] = h0_ref[2]
    c_all1[pl.ds(2 * r, 2)] = c0_ref[core]
    c_all2[pl.ds(2 * r, 2)] = c0_ref[2]

    for n, (src, use) in enumerate(jobs):
        def body(i, c):
            slot = lax.rem(i, STAGES)
            nbytes_wait(stage.at[slot], stage_sem.at[slot])
            ahead = i + STAGES - 1
            slot_ahead = lax.rem(ahead, STAGES)

            @pl.when(ahead < n_row)
            def _():
                load(src, ahead, slot_ahead)

            @pl.when(ahead >= n_row)
            def _():
                load(jobs[n + 1][0] if n + 1 < len(jobs) else w_h2, ahead - n_row, slot_ahead)
            use(*group_of(i), sorted_tile(slot))
            return c
        lax.fori_loop(0, n_row, body, 0)
        if n == 2:
            @pl.when(core == 1)
            def _():
                remote(p_f, xz_in, pf_send, pf_sem, mate, y).start()

    nbytes_wait(hs1.at[0, pl.ds(0, 2 * n_row - 2)], h0_sem.at[0])
    nbytes_wait(hs2.at[0, pl.ds(0, 2 * n_row - 2)], h0_sem.at[1])
    nbytes_wait(c_all1.at[pl.ds(0, 2 * n_row - 2)], c0_sem.at[0])
    nbytes_wait(c_all2.at[pl.ds(0, 2 * n_row - 2)], c0_sem.at[1])

    def own_state(c_all):
        for hf in range(2):
            c_st[hf] = c_all[own_j, :, hf * unit:(hf + 1) * unit]
    own_state(c_all1)

    def rows_of(t):
        return pl.ds(pl.multiple_of(lax.rem(t, BATCH) * PAD, PAD), PAD)

    def cell(acc, hs, new):
        h_new = []
        for hf in range(2):
            gate = [acc[hf][:, k * unit:(k + 1) * unit] for k in range(4)]
            c = (jax.nn.sigmoid(gate[1]) * c_st[hf]
                 + jax.nn.sigmoid(gate[0]) * jnp.tanh(gate[2]))
            c_st[hf] = c
            h = (jax.nn.sigmoid(gate[3]) * jnp.tanh(c)).astype(BF16)
            hs[new, own_j, :, hf * unit:(hf + 1) * unit] = h
            h_new.append(h)
        return h_new

    def to_mate(slot):
        time = slot - 1 + core
        return remote(hs1.at[slot, pl.ds(2 * mate, 2)], h_oth.at[time], fwd_send,
                      fwd_sem.at[(1 - core) * lax.div(time, BATCH)], mate, y)

    def mid(m):
        for i in range(BATCH):
            for jj in range(2):
                here = slice(i * PAD, (i + 1) * PAD), slice(jj * chunk, (jj + 1) * chunk)
                lhs[0, here[0], here[1]] = hs1[m * BATCH + i + 1 - core, 2 * r + jj].astype(F32)
                lhs[1, here[0], here[1]] = h_oth[m * BATCH + i, jj].astype(F32)
        left, right = lhs[0].astype(BF16), lhs[1].astype(BF16)

        def one(k, c):
            tx = lax.rem(x + k, n_x)
            for hf in range(2):
                g = 2 * tx + hf
                p_b[m, tx, hf] = (jnp.dot(left, w_mid[core, g], preferred_element_type=F32)
                                  + jnp.dot(right, w_mid[1 - core, g], preferred_element_type=F32))

            @pl.when(jnp.logical_or(k > 0, core == 0))
            def _():
                remote(p_b.at[m, tx], z_in.at[m, 2 * lax.rem(n_x - k, n_x) + core], mid_send, z_sem.at[m],
                       2 * tx + 1, y).start()
            return c
        lax.fori_loop(0, n_x, one, 0)

    groups = hop_groups(n_x, n_col)
    offsets = [o for grp in groups for o in grp]
    index = {o: i for i, o in enumerate(offsets)}

    def chain_step(hs, w, prev, new, s, z_of, b_ref, last_send, in_wait, after_receive):
        parity = lax.rem(s, 2)
        acc = [z_of(hf) + b_ref[2 * x + hf] for hf in range(2)]
        for n, grp in enumerate(groups):
            if n:
                @pl.when(s > 0)
                def _():
                    for dx, dy in grp:
                        j = lax.rem(y + dy, n_col) * n_x + lax.rem(x + dx, n_x)
                        nbytes_wait(hs.at[prev, j], step_sem.at[1 - parity, index[dx, dy]])
            if n == len(groups) - 1:
                after_receive()
            for dx, dy in grp:
                j = lax.rem(y + dy, n_col) * n_x + lax.rem(x + dx, n_x)
                h = hs[prev, j]
                rows = pl.ds(pl.multiple_of(lax.rem(j, 2) * chunk, chunk), chunk)
                for hf in range(2):
                    acc[hf] += jnp.dot(h, w[lax.div(j, 2), hf, rows], preferred_element_type=F32)
            if n == 0:
                in_wait()
        h_new = cell(acc, hs, new)

        def send():
            for dx, dy in reversed(offsets[1:]):
                remote(hs.at[new, own_j], hs.at[new, own_j], step_send,
                       step_sem.at[parity, index[(n_x - dx) % n_x, (n_col - dy) % n_col]],
                       2 * lax.rem(x + dx, n_x) + 1, lax.rem(y + dy, n_col)).start()
        if last_send:
            send()
        else:
            pl.when(s < n_step - 1)(send)
        return h_new

    @pl.when(core == 1)
    def _():
        for m in reversed(range(n_bat)):
            remote(p_b.at[m], z_in.at[m, pl.ds(0, n_x)], pb_send, pb_sem.at[m], mate, y).start()

        def tiles(n, c):
            late_tile(n)
            return c
        lax.fori_loop(0, 3 * n_row, tiles, 0)
        nbytes_wait(w_one.at[pl.ds(0, n_row - 1)], w_sem.at[0])

        def step_one(s, c):
            t = n_step - 1 - s
            m, rows = lax.div(t, BATCH), rows_of(t)

            @pl.when(lax.rem(t, BATCH) == BATCH - 1)
            def _():
                nbytes_wait(xz_in.at[m], xz_sem.at[m])

            def z_of(hf):
                z = xz_in[m, 0, hf, rows]
                for d in range(1, n_x):
                    z = z + xz_in[m, d, hf, rows]
                return z

            def pass_on():
                @pl.when(s > 0)
                def _():
                    to_mate(t + 1).start()
            chain_step(hs1, w_one, t + 1, t, s, z_of, b1_ref.at[1], True, lambda: None, pass_on)
            piece(2 * s)
            piece(2 * s + 1)
            return c
        lax.fori_loop(0, n_step, step_one, 0)
        for dx, dy in offsets[1:]:
            j = lax.rem(y + dy, n_col) * n_x + lax.rem(x + dx, n_x)
            nbytes_wait(hs1.at[0, j], step_sem.at[(n_step - 1) % 2, index[dx, dy]])
        to_mate(0).start()
        co[1] = c_st[0]
        out_c[1] = c_st[1]
        own_state(c_all2)
        nbytes_wait(p_b, pb_send)

        def mid_north(m):
            nbytes_wait(h_oth.at[pl.ds(m * BATCH, BATCH)], fwd_sem.at[m])
            mid(m)

        def early(m, c):
            mid_north(m)
            return c
        lax.fori_loop(0, 2, early, 0)
        nbytes_wait(w_two.at[pl.ds(0, n_row - 1)], w_sem.at[1])

        def step_two(t, c):
            m, rows = lax.div(t, BATCH), rows_of(t)

            @pl.when(lax.rem(t, BATCH) == 0)
            def _():
                nbytes_wait(z_in.at[m, pl.ds(0, n_row - 1)], z_sem.at[m])

            def z_of(hf):
                z = p_b[m, x, hf, rows]
                for d in range(n_row):
                    if d != 1:
                        z = z + z_in[m, d, hf, rows]
                return z

            def in_wait():
                late = n_step - 4 * BATCH

                @pl.when(jnp.logical_and(lax.rem(t, BATCH) == 0, jnp.logical_and(t != late, t < n_step - BATCH)))
                def _():
                    mid_north(m + jnp.where(t < late, 2, 1))
            h_new = chain_step(hs2, w_two, t, t + 1, t, z_of, b2_ref, False, in_wait, lambda: None)
            ho[t] = h_new[0]
            out_h[t] = h_new[1]
            return c
        lax.fori_loop(0, n_step, step_two, 0)
        co[2] = c_st[0]
        out_c[2] = c_st[1]
        ends = [remote(ho, out_h, end_send.at[0], end_sem.at[0], mate, y),
                remote(co.at[pl.ds(1, 2)], out_c.at[pl.ds(1, 2)], end_send.at[1], end_sem.at[1], mate, y)]
        for e in ends:
            e.start()
        for e in ends:
            e.wait_send()
        nbytes_wait(out_c.at[0], end_sem.at[2])
        nbytes_wait(hs1.at[pl.ds(0, n_step), pl.ds(0, n_x * n_col - 1)], step_send)
        nbytes_wait(hs2.at[pl.ds(0, n_step - 1), pl.ds(0, n_x * n_col - 1)], step_send)
        nbytes_wait(p_b.at[:, pl.ds(0, n_x - 1)], mid_send)
        nbytes_wait(p_f, pf_send)
        nbytes_wait(w_fwd.at[0], f_send)
        nbytes_wait(send_a.at[pl.ds(0, n_row - 2)], a_send)
        nbytes_wait(send_c.at[pl.ds(0, n_row - 2)], c_send)

    @pl.when(core == 0)
    def _():
        def add(i, c):
            m = n_bat - 1 - i
            nbytes_wait(z_in.at[m, pl.ds(0, n_x)], pb_sem.at[m])
            for d in range(n_x):
                tx = lax.rem(x + d, n_x)
                p_b[m, tx] += z_in[m, tx]
                remote(p_b.at[m, tx], xz_in.at[m, (n_x - d) % n_x], xz_send, xz_sem.at[m], 2 * tx + 1, y).start()
            return c
        lax.fori_loop(0, n_bat, add, 0)
        nbytes_wait(xz_in, pf_sem)
        nbytes_wait(w_fwd.at[1], f_sem)
        first_mid = n_step - 10

        def receive_rows(slot, parity):
            for k in range(n_x):
                @pl.when(jnp.logical_or(x != k, x != y))
                def _():
                    nbytes_wait(hs1.at[slot, x * n_x + k], row_sem.at[parity, k])

        def step_fwd(t, c):
            m, rows, parity = lax.div(t, BATCH), rows_of(t), lax.rem(t, 2)

            @pl.when(t > 0)
            def _():
                receive_rows(t, 1 - parity)
                to_mate(t).start()
            hv = [hs1[t, x * n_x + k] for k in range(n_x)]
            for d in (1, 3, 2, 0):
                tx = lax.rem(x + d, n_x)
                for hf in range(2):
                    acc = p_f[m, tx, hf, rows] + xz_in[m, tx, hf, rows]
                    for k in range(n_x):
                        acc += jnp.dot(hv[k], w_fwd[k // 2, 2 * tx + hf, (k % 2) * chunk:(k % 2 + 1) * chunk],
                                       preferred_element_type=F32)
                    z_out[parity, tx, hf] = acc
                if d:
                    remote(z_out.at[parity, tx], z_part.at[parity, n_x - 1 - d], part_send,
                           part_sem.at[parity, n_x - 1 - d], 2 * tx, y).start()

            @pl.when(t < 3 * n_row // 2)
            def _():
                late_tile(2 * t)

            @pl.when(t == first_mid)
            def _():
                nbytes_wait(h_oth, fwd_sem.at[0])
                nbytes_wait(p_b, xz_send)

            @pl.when(jnp.logical_and(t >= first_mid, jnp.logical_or(t < first_mid + 4, lax.rem(t, 2) == 0)))
            def _():
                mid(jnp.where(t < first_mid + 4, 2 * (t - first_mid), lax.div(t, 2) - 1))

            for d in range(n_x - 1):
                nbytes_wait(z_part.at[parity, d], part_sem.at[parity, d])
            acc = []
            for hf in range(2):
                z = z_out[parity, x, hf] + b1_ref[0, 2 * x + hf]
                for d in range(n_x - 1):
                    z = z + z_part[parity, d, hf]
                acc.append(z)
            cell(acc, hs1, t + 1)
            for k in range(n_col):
                to_y = lax.rem(y + k, n_col)

                def give():
                    remote(hs1.at[t + 1, own_j], hs1.at[t + 1, own_j], step_send, row_sem.at[parity, x],
                           2 * y, to_y).start()
                if k:
                    give()
                else:
                    pl.when(x != y)(give)

            @pl.when(t < 3 * n_row // 2)
            def _():
                late_tile(2 * t + 1)

            @pl.when(jnp.logical_and(t >= 1, t < 1 + 3 * PIECES // 2))
            def _():
                for k in range(4):
                    piece(4 * (t - 1) + k)

            @pl.when(jnp.logical_and(t >= first_mid, t < first_mid + 4))
            def _():
                mid(2 * (t - first_mid) + 1)
            nbytes_wait(z_out.at[0, pl.ds(0, n_x - 1)], part_send)
            return c
        lax.fori_loop(0, n_step, step_fwd, 0)
        receive_rows(n_step, (n_step - 1) % 2)
        to_mate(n_step).start()
        mid(n_bat - 1)
        out_c[0] = c_st[0]
        co[0] = c_st[1]
        e = remote(co.at[0], out_c.at[0], end_send.at[2], end_sem.at[2], mate, y)
        e.start()
        e.wait_send()
        nbytes_wait(out_h, end_sem.at[0])
        nbytes_wait(out_c.at[pl.ds(1, 2)], end_sem.at[1])
        nbytes_wait(p_b, mid_send)
        nbytes_wait(send_a, a_send)
        nbytes_wait(send_c, c_send)
        nbytes_wait(hs1.at[pl.ds(0, n_step), pl.ds(0, n_col - 1)], step_send)

        @pl.when(x != y)
        def _():
            nbytes_wait(hs1.at[pl.ds(0, n_step), 0], step_send)

    nbytes_wait(h_oth, fwd_send)
    nbytes_wait(hs1.at[0, pl.ds(0, 2 * n_row - 2)], init_send)
    nbytes_wait(hs1.at[0, pl.ds(0, 2 * n_row - 2)], init_send)
    nbytes_wait(c_all1.at[pl.ds(0, 2 * n_row - 2)], init_send)
    nbytes_wait(c_all1.at[pl.ds(0, 2 * n_row - 2)], init_send)


def solution(mesh):
    n_row = mesh.shape['row']
    n_col = mesh.shape['col']
    spec_seq = P(None, 'data', 'row')
    spec_weight = P(None, 'row', 'col')
    spec_out = P(None, 'data', ('col', 'row'))

    def local(x_rows, w_x1, w_h1, b_1, w_x2, w_h2, b_2, h_zero, c_zero):
        n_step, batch, deep = x_rows.shape
        cols = w_h2.shape[1]
        wide = cols // n_row
        unit = wide // 4
        n_chunk = n_row // 2 * n_col
        chunk = 2 * unit
        n_bat = n_step // BATCH
        n_x = n_row // 2

        def padded(v):
            return jnp.pad(v, ((0, 0), (0, PAD - batch), (0, 0)))

        def by_chunk(v):
            return padded(v).reshape(3, PAD, 2, chunk).transpose(0, 2, 1, 3)

        x_in = padded(x_rows).reshape(n_step * PAD, deep)
        h_in = by_chunk(h_zero.astype(BF16))
        c_in = by_chunk(c_zero)
        bias1 = b_1.reshape(2, n_row, unit, 4).transpose(0, 1, 3, 2).reshape(2, n_row, 1, wide)
        bias2 = b_2.reshape(n_row, unit, 4).transpose(0, 2, 1).reshape(n_row, 1, wide)
        vmem = pl.BlockSpec(memory_space=pltpu.VMEM)
        hbm = pl.BlockSpec(memory_space=pl.ANY)
        dma = pltpu.SemaphoreType.DMA
        rows = BATCH * PAD
        weights = (n_row, 2, deep, wide)
        h_out, c_out = pl.pallas_call(
            functools.partial(kernel, n_row, n_col),
            out_shape=(jax.ShapeDtypeStruct((n_step, PAD, unit), BF16),
                       jax.ShapeDtypeStruct((3, PAD, unit), F32)),
            in_specs=[vmem] * 5 + [hbm] * 4,
            out_specs=(vmem, vmem),
            scratch_shapes=[
                pltpu.VMEM(weights, BF16),
                pltpu.VMEM(weights, BF16),
                pltpu.VMEM((2, n_row, deep, wide), BF16),
                pltpu.VMEM((2, n_row, deep, wide), BF16),
                pltpu.VMEM((n_row, deep, wide), BF16),
                pltpu.VMEM((n_row, deep, wide), BF16),
                pltpu.VMEM((STAGES, deep, wide), BF16),
                pltpu.VMEM((wide, wide), BF16),
                pltpu.VMEM((n_bat, n_x, 2, rows, wide), F32),
                pltpu.VMEM((n_bat, n_x, 2, rows, wide), F32),
                pltpu.VMEM((n_bat, n_x, 2, rows, wide), F32),
                pltpu.VMEM((n_bat, n_row, 2, rows, wide), F32),
                pltpu.VMEM((2, n_x, 2, PAD, wide), F32),
                pltpu.VMEM((2, n_x - 1, 2, PAD, wide), F32),
                pltpu.VMEM((2, rows, deep), F32),
                pltpu.VMEM((n_step + 1, n_chunk, PAD, chunk), BF16),
                pltpu.VMEM((n_step + 1, n_chunk, PAD, chunk), BF16),
                pltpu.VMEM((n_step, 2, PAD, chunk), BF16),
                pltpu.VMEM((n_chunk, PAD, chunk), F32),
                pltpu.VMEM((n_chunk, PAD, chunk), F32),
                pltpu.VMEM((2, PAD, unit), F32),
                pltpu.VMEM((n_step, PAD, unit), BF16),
                pltpu.VMEM((3, PAD, unit), F32),
                dma((STAGES,)), dma(()), dma((2,)),
                dma(()), dma(()), dma(()),
                dma(()), dma(()), dma(()), dma((n_bat,)),
                dma(()), dma((n_bat,)), dma(()), dma((n_bat,)),
                dma(()), dma((2,)), dma((2,)),
                dma(()), dma((2, n_chunk)),
                dma(()), dma((2, n_x - 1)), dma((2, n_x)),
                dma(()), dma((n_bat,)),
                dma((3,)), dma((3,)),
            ],
            compiler_params=pltpu.CompilerParams(collective_id=0, has_side_effects=True,
                                                 vmem_limit_bytes=67_043_328),
        )(x_in, h_in, c_in, bias1, bias2, w_x1, w_h1, w_x2, w_h2)
        return h_out[:, :batch], c_out[:, :batch]

    return jax.shard_map(local, mesh=mesh,
                         in_specs=(spec_seq, spec_weight, spec_weight, P(None, 'col'), spec_weight,
                                   P('row', 'col'), P('col'), spec_seq, spec_seq),
                         out_specs=(spec_out, spec_out), check_vma=False)
```

```python
import functools

import jax
import jax.numpy as jnp
from jax import lax
from jax.experimental import pallas as pl
from jax.experimental.pallas import tpu as pltpu
from jax.sharding import PartitionSpec as P

PAD = 8
STAGES = 4
BATCH = 2
PIECES = 8
F32, BF16 = jnp.float32, jnp.bfloat16


def nbytes_wait(ref, sem):
    pltpu.make_async_copy(ref, ref, sem).wait()


def hop_groups(n_x, n_y):
    far = {}
    for dy in range(n_y):
        for dx in range(n_x):
            far.setdefault(min(dx, n_x - dx) + min(dy, n_y - dy), []).append((dx, dy))
    return [far[k] for k in sorted(far)]


def kernel(n_row, n_col, x_in, h_in, c_in, b1_in, b2_in, w_x1, w_h1, w_x2, w_h2, out_h, out_c,
           x_ref, h0_ref, c0_ref, bias, w_one, w_two, w_fwd, w_mid, send_a, send_c, stage, sort, p_b, p_f, xz_in, z_in, z_out, z_part, lhs,
           hs1, hs2, h_oth, c_all1, c_all2, c_st, ho, co,
           stage_sem, a_send, pass_sem, w_sem, f_send, f_sem, m_sem, c_send, pf_send, pf_sem, pb_send, pb_sem, xz_send, xz_sem,
           mid_send, z_sem, init_send, h0_sem, c0_sem, step_send, step_sem, part_send, part_sem, row_sem,
           fwd_send, fwd_sem, end_send, end_sem):
    n_x = n_row // 2
    batch, n_step = x_in.shape[:2]
    n_bat = n_step // BATCH
    deep = w_h2.shape[0]
    wide = w_h2.shape[1] // n_row
    unit = wide // 4
    chunk = deep // 2
    r = lax.axis_index('row')
    y = lax.axis_index('col')
    core = lax.rem(r, 2)
    x = lax.div(r, 2)
    mate = r + 1 - 2 * core
    own_j = y * n_x + x

    def at(row, col):
        return {'row': row, 'col': col}

    def remote(src, dst, ssem, rsem, row, col):
        return pltpu.make_async_remote_copy(src_ref=src, dst_ref=dst, send_sem=ssem, recv_sem=rsem,
                                            device_id=at(row, col), device_id_type=pl.DeviceIdType.MESH)

    def group_of(i):
        near = jnp.logical_and(i >= 2, i < 6)
        dx = jnp.where(near, 1 + 2 * lax.rem(i, 2), jnp.where(i < 2, 2, 0))
        half = jnp.where(near, lax.div(i - 2, 2), lax.rem(i, 2))
        return lax.rem(x + dx, n_x), half

    def load(src, i, slot):
        tx, half = group_of(i)
        first = pl.multiple_of((2 * tx + half) * wide, wide)
        pltpu.make_async_copy(src.at[:, pl.ds(first, wide)], stage.at[slot], stage_sem.at[slot]).start()

    def load_late(n):
        slot, i = lax.rem(n, STAGES), lax.rem(n, n_row)

        @pl.when(n < n_row)
        def _():
            load(w_h2, i, slot)

        @pl.when(jnp.logical_and(n >= n_row, n < 3 * n_row))
        def _():
            load(w_x2.at[lax.div(n - n_row, n_row)], i, slot)

    def sorted_tile(slot):
        return jnp.dot(stage[slot], sort[...], preferred_element_type=F32).astype(BF16)

    def use_back(i, tile):
        tx, half = group_of(i)
        g = 2 * tx + half

        @pl.when(jnp.logical_and(tx == x, core == 1))
        def _():
            w_one[r, half] = tile

        @pl.when(jnp.logical_or(tx != x, core == 0))
        def _():
            send_a[g] = tile

        @pl.when(jnp.logical_and(tx != x, core == 1))
        def _():
            remote(send_a.at[g], w_one.at[r, half], a_send, w_sem.at[0], 2 * tx + 1, y).start()

        @pl.when(jnp.logical_and(tx != x, core == 0))
        def _():
            remote(send_a.at[g], w_fwd.at[1, g], a_send, pass_sem.at[i], mate, y).start()

        @pl.when(jnp.logical_and(tx == x, core == 0))
        def _():
            remote(send_a.at[g], w_one.at[r, half], a_send, w_sem.at[0], mate, y).start()

    def pass_back(i, c):
        tx, half = group_of(i)
        g = 2 * tx + half
        nbytes_wait(w_fwd.at[1, g], pass_sem.at[i])
        remote(w_fwd.at[1, g], w_one.at[mate, half], a_send, w_sem.at[0], 2 * tx + 1, y).start()
        return c

    def use_fwd(i, tile):
        tx, half = group_of(i)
        g = 2 * tx + half
        w_fwd[0, g] = tile

        @pl.when(core == 1)
        def _():
            remote(w_fwd.at[0, g], w_fwd.at[1, g], f_send, f_sem, mate, y).start()

    def project(buf):
        def use(i, tile):
            tx, half = group_of(i)
            z = jnp.dot(x_ref[...], tile, preferred_element_type=F32)
            for m in range(n_bat):
                buf[m, tx, half] = z[m * BATCH * PAD:(m + 1) * BATCH * PAD]
        return use

    def late_tile(n):
        slot = lax.rem(n, STAGES)
        nbytes_wait(stage.at[slot], stage_sem.at[slot])
        load_late(n + STAGES - 1)
        tile = sorted_tile(slot)
        tx, half = group_of(lax.rem(n, n_row))
        g = 2 * tx + half

        @pl.when(n >= n_row)
        def _():
            k = lax.div(n - n_row, n_row)
            w_mid[k, g] = tile

            @pl.when(core == 1)
            def _():
                remote(w_mid.at[k, g], w_two.at[g, k], f_send, m_sem, mate, y).start()

        @pl.when(jnp.logical_and(n < n_row, jnp.logical_and(tx == x, core == 1)))
        def _():
            w_two[r, half] = tile

        @pl.when(jnp.logical_and(n < n_row, jnp.logical_or(tx != x, core == 0)))
        def _():
            send_c[g] = tile

        @pl.when(jnp.logical_and(n < n_row, jnp.logical_and(tx == x, core == 0)))
        def _():
            remote(send_c.at[g], w_two.at[r, half], c_send, w_sem.at[1], mate, y).start()

    def piece(p):
        half, q = lax.div(p, 3 * PIECES), lax.rem(p, 3 * PIECES)
        k, e = lax.div(q, 3), lax.rem(q, 3)
        tx = lax.rem(x + jnp.where(e < 2, 1 + 2 * e, 2), n_x)
        n_rows = deep // PIECES
        rows = pl.ds(pl.multiple_of(k * n_rows, n_rows), n_rows)
        remote(send_c.at[2 * tx + half, rows], w_two.at[r, half, rows], c_send, w_sem.at[1], 2 * tx + 1, y).start()

    jobs = [(w_h1.at[1], use_back), (w_h1.at[0], use_fwd), (w_x1.at[0], project(p_f)), (w_x1.at[1], project(p_b))]
    for i in range(STAGES - 1):
        load(jobs[0][0], i, i)
    barrier = pltpu.get_barrier_semaphore()
    for dc in range(n_col):
        for dr in range(n_row):
            if dc or dr:
                pl.semaphore_signal(barrier, inc=1, device_id=at(lax.rem(r + dr, n_row), lax.rem(y + dc, n_col)),
                                    device_id_type=pl.DeviceIdType.MESH)

    def iota2(shape):
        return lax.broadcasted_iota(jnp.int32, shape, 0), lax.broadcasted_iota(jnp.int32, shape, 1)

    rows_i, cols_i = iota2((wide, wide))
    gate_i, unit_i = lax.div(cols_i, unit), lax.rem(cols_i, unit)
    sort[...] = jnp.where(rows_i == 4 * unit_i + gate_i, 1.0, 0.0).astype(BF16)

    for k in range(3):
        lhs[0, 0:PAD, 0:deep] = jnp.zeros((PAD, deep), F32)
        lhs[0, 0:batch, 0:deep] = h_in[k]
        for jj in range(2):
            here = slice(jj * chunk, (jj + 1) * chunk)
            h0_ref[k, jj] = lhs[0, 0:PAD, here].astype(BF16)
            c0_ref[k, jj] = jnp.zeros((PAD, chunk), F32)
            c0_ref[k, jj, 0:batch] = c_in[k, :, here]

    pl.semaphore_wait(barrier, n_col * n_row - 1)

    for d in range(1, n_row):
        to = lax.rem(r + d, n_row)
        tc = lax.rem(to, 2)
        here = pl.ds(2 * r, 2)
        remote(h0_ref.at[tc], hs1.at[tc * n_step, here], init_send, h0_sem.at[0], to, y).start()
        remote(h0_ref.at[2], hs2.at[0, here], init_send, h0_sem.at[1], to, y).start()
        remote(c0_ref.at[tc], c_all1.at[here], init_send, c0_sem.at[0], to, y).start()
        remote(c0_ref.at[2], c_all2.at[here], init_send, c0_sem.at[1], to, y).start()
    hs1[core * n_step, pl.ds(2 * r, 2)] = h0_ref[core]
    hs2[0, pl.ds(2 * r, 2)] = h0_ref[2]
    c_all1[pl.ds(2 * r, 2)] = c0_ref[core]
    c_all2[pl.ds(2 * r, 2)] = c0_ref[2]

    def prepare():
        for hf in range(2):
            cols = pl.ds(pl.multiple_of((2 * x + hf) * wide, wide), wide)
            for n, b_row in enumerate((b1_in[pl.ds(core, 1), cols], b2_in[:, cols])):
                left = jnp.broadcast_to(b_row * 0.5, (PAD, wide))
                total = jnp.zeros((PAD, wide), F32)
                for _ in range(3):
                    part = left.astype(BF16)
                    total += jnp.dot(part, sort[...], preferred_element_type=F32)
                    left = left - part.astype(F32)
                bias[n, hf] = total * 2.0

        rows_i, cols_i = iota2((n_step * PAD, batch * n_step))
        take = jnp.where(cols_i == lax.rem(rows_i, PAD) * n_step + lax.div(rows_i, PAD), 1.0, 0.0)
        take = jnp.where(lax.rem(rows_i, PAD) < batch, take, 0.0).astype(BF16)
        flat = x_in[...].astype(F32).reshape(batch * n_step, deep).astype(BF16)
        x_ref[...] = jnp.dot(take, flat, preferred_element_type=F32).astype(BF16)

    for n, (src, use) in enumerate(jobs):
        def body(i, c):
            slot = lax.rem(i, STAGES)
            nbytes_wait(stage.at[slot], stage_sem.at[slot])
            ahead = i + STAGES - 1
            slot_ahead = lax.rem(ahead, STAGES)

            @pl.when(ahead < n_row)
            def _():
                load(src, ahead, slot_ahead)

            @pl.when(ahead >= n_row)
            def _():
                load(jobs[n + 1][0] if n + 1 < len(jobs) else w_h2, ahead - n_row, slot_ahead)
            use(i, sorted_tile(slot))
            return c
        lax.fori_loop(0, n_row, body, 0)
        if n == 0:
            @pl.when(core == 1)
            def _():
                lax.fori_loop(0, n_row - 2, pass_back, 0)
            prepare()
        if n == 2:
            @pl.when(core == 1)
            def _():
                remote(p_f, xz_in, pf_send, pf_sem, mate, y).start()

    nbytes_wait(hs1.at[0, pl.ds(0, 2 * n_row - 2)], h0_sem.at[0])
    nbytes_wait(hs2.at[0, pl.ds(0, 2 * n_row - 2)], h0_sem.at[1])
    nbytes_wait(c_all1.at[pl.ds(0, 2 * n_row - 2)], c0_sem.at[0])
    nbytes_wait(c_all2.at[pl.ds(0, 2 * n_row - 2)], c0_sem.at[1])

    def own_state(c_all):
        for hf in range(2):
            c_st[hf] = c_all[own_j, :, hf * unit:(hf + 1) * unit]
    own_state(c_all1)

    def rows_of(t):
        return pl.ds(pl.multiple_of(lax.rem(t, BATCH) * PAD, PAD), PAD)

    def cell(acc, hs, new):
        h_new = []
        for hf in range(2):
            gate = [acc[hf][:, k * unit:(k + 1) * unit] for k in range(4)]
            c = (jax.nn.sigmoid(gate[1]) * c_st[hf]
                 + jax.nn.sigmoid(gate[0]) * jnp.tanh(gate[2]))
            c_st[hf] = c
            h = (jax.nn.sigmoid(gate[3]) * jnp.tanh(c)).astype(BF16)
            hs[new, own_j, :, hf * unit:(hf + 1) * unit] = h
            h_new.append(h)
        return h_new

    def to_mate(slot):
        return remote(hs1.at[slot, pl.ds(x * n_x, n_x)], h_oth.at[slot], fwd_send, fwd_sem, mate, y)

    def mid(m):
        for i in range(BATCH):
            for jj in range(n_x):
                here = slice(i * PAD, (i + 1) * PAD), slice(jj * chunk, (jj + 1) * chunk)
                lhs[0, here[0], here[1]] = hs1[m * BATCH + i + 1, x * n_x + jj].astype(F32)
                lhs[1, here[0], here[1]] = h_oth[m * BATCH + i, jj].astype(F32)
        left = [[lhs[k, :, c * deep:(c + 1) * deep].astype(BF16) for c in range(2)] for k in range(2)]

        def one(d, c):
            tx = lax.rem(x + d, n_x)
            for hf in range(2):
                g = 2 * tx + hf
                z = jnp.dot(left[0][0], w_mid[0, g], preferred_element_type=F32)
                z += jnp.dot(left[1][0], w_mid[1, g], preferred_element_type=F32)
                z += jnp.dot(left[0][1], w_two[g, 0], preferred_element_type=F32)
                z += jnp.dot(left[1][1], w_two[g, 1], preferred_element_type=F32)
                p_b[m, tx, hf] = z
            remote(p_b.at[m, tx], z_in.at[m, lax.rem(n_x - d, n_x)], mid_send, z_sem.at[m], 2 * tx + 1, y).start()
            return c
        lax.fori_loop(0, n_x, one, 0)

    groups = hop_groups(n_x, n_col)
    offsets = [o for grp in groups for o in grp]
    index = {o: i for i, o in enumerate(offsets)}

    def chain_step(hs, w, prev, new, s, z_of, layer, last_send, after_receive):
        parity = lax.rem(s, 2)
        acc = [z_of(hf) + bias[layer, hf] for hf in range(2)]
        for n, grp in enumerate(groups):
            if n:
                @pl.when(s > 0)
                def _():
                    for dx, dy in grp:
                        j = lax.rem(y + dy, n_col) * n_x + lax.rem(x + dx, n_x)
                        nbytes_wait(hs.at[prev, j], step_sem.at[1 - parity, index[dx, dy]])
            if n == len(groups) - 1:
                after_receive()
            for dx, dy in grp:
                j = lax.rem(y + dy, n_col) * n_x + lax.rem(x + dx, n_x)
                h = hs[prev, j]
                rows = pl.ds(pl.multiple_of(lax.rem(j, 2) * chunk, chunk), chunk)
                for hf in range(2):
                    acc[hf] += jnp.dot(h, w[lax.div(j, 2), hf, rows], preferred_element_type=F32)
        h_new = cell(acc, hs, new)

        def send():
            for dx, dy in reversed(offsets[1:]):
                remote(hs.at[new, own_j], hs.at[new, own_j], step_send,
                       step_sem.at[parity, index[(n_x - dx) % n_x, (n_col - dy) % n_col]],
                       2 * lax.rem(x + dx, n_x) + 1, lax.rem(y + dy, n_col)).start()
        if last_send:
            send()
        else:
            pl.when(s < n_step - 1)(send)
        return h_new

    @pl.when(core == 1)
    def _():
        def send_batch(m):
            for d in (2, 1, 3):
                tx = lax.rem(x + d, n_x)
                remote(p_b.at[m, tx], xz_in.at[m, n_x - 1 - d], xz_send, xz_sem.at[m], 2 * tx + 1, y).start()

        def add(i, c):
            m = n_bat - 1 - i
            nbytes_wait(z_in.at[m], pb_sem.at[m])
            for tx in range(n_x):
                p_b[m, tx] += z_in[m, tx]

            @pl.when(i < 2)
            def _():
                send_batch(m)
            return c
        lax.fori_loop(0, n_bat, add, 0)

        def tiles(n, c):
            late_tile(n)
            return c
        lax.fori_loop(0, 3 * n_row, tiles, 0)
        nbytes_wait(w_one.at[pl.ds(0, n_row - 1)], w_sem.at[0])

        def step_one(s, c):
            t = n_step - 1 - s
            m, rows = lax.div(t, BATCH), rows_of(t)

            @pl.when(lax.rem(t, BATCH) == BATCH - 1)
            def _():
                nbytes_wait(xz_in.at[m, pl.ds(0, n_x - 1)], xz_sem.at[m])

            def z_of(hf):
                z = p_b[m, x, hf, rows]
                for d in range(n_x - 1):
                    z = z + xz_in[m, d, hf, rows]
                return z

            def pass_on():
                @pl.when(s > 0)
                def _():
                    to_mate(t + 1).start()
            chain_step(hs1, w_one, t + 1, t, s, z_of, 0, True, pass_on)

            @pl.when(jnp.logical_and(lax.rem(s, 2) == 0, s < n_step - 4))
            def _():
                send_batch(n_bat - 3 - lax.div(s, 2))
            piece(2 * s - lax.rem(s, 2))

            @pl.when(lax.rem(s, 2) == 1)
            def _():
                piece(2 * s)
                piece(2 * s + 1)
            return c
        lax.fori_loop(0, n_step, step_one, 0)
        for dx, dy in offsets[1:]:
            j = lax.rem(y + dy, n_col) * n_x + lax.rem(x + dx, n_x)
            nbytes_wait(hs1.at[0, j], step_sem.at[(n_step - 1) % 2, index[dx, dy]])
        to_mate(0).start()
        co[1] = c_st[0]
        out_c[1] = c_st[1]
        own_state(c_all2)
        nbytes_wait(w_two.at[pl.ds(0, n_row - 1)], w_sem.at[1])

        def step_two(t, c):
            m, rows = lax.div(t, BATCH), rows_of(t)

            @pl.when(lax.rem(t, BATCH) == 0)
            def _():
                nbytes_wait(z_in.at[m], z_sem.at[m])

            def z_of(hf):
                z = z_in[m, 0, hf, rows]
                for d in range(1, n_x):
                    z = z + z_in[m, d, hf, rows]
                return z
            h_new = chain_step(hs2, w_two, t, t + 1, t, z_of, 1, False, lambda: None)
            ho[t] = h_new[0]
            out_h[t] = h_new[1]
            return c
        lax.fori_loop(0, n_step, step_two, 0)
        co[2] = c_st[0]
        out_c[2] = c_st[1]
        ends = [remote(ho, out_h, end_send.at[0], end_sem.at[0], mate, y),
                remote(co.at[pl.ds(1, 2)], out_c.at[pl.ds(1, 2)], end_send.at[1], end_sem.at[1], mate, y)]
        for e in ends:
            e.start()
        for e in ends:
            e.wait_send()
        nbytes_wait(out_c.at[0], end_sem.at[2])
        nbytes_wait(hs1.at[pl.ds(0, n_step), pl.ds(0, n_x * n_col - 1)], step_send)
        nbytes_wait(hs2.at[pl.ds(0, n_step - 1), pl.ds(0, n_x * n_col - 1)], step_send)
        nbytes_wait(p_b.at[:, pl.ds(0, n_x - 1)], xz_send)
        nbytes_wait(h_oth, fwd_send)
        nbytes_wait(p_f, pf_send)
        nbytes_wait(w_fwd.at[0], f_send)
        nbytes_wait(w_mid, f_send)
        nbytes_wait(send_a.at[pl.ds(0, n_row - 2)], a_send)
        nbytes_wait(send_a.at[pl.ds(0, n_row - 2)], a_send)
        nbytes_wait(send_c.at[pl.ds(0, n_row - 2)], c_send)

    @pl.when(core == 0)
    def _():
        for m in reversed(range(n_bat)):
            remote(p_b.at[m], z_in.at[m], pb_send, pb_sem.at[m], mate, y).start()
        nbytes_wait(xz_in, pf_sem)
        nbytes_wait(w_fwd.at[1], f_sem)
        first_mid = n_step - 11

        def receive_rows(slot, parity):
            for k in range(n_x):
                @pl.when(jnp.logical_or(x != k, x != y))
                def _():
                    nbytes_wait(hs1.at[slot, x * n_x + k], row_sem.at[parity, k])

        def step_fwd(t, c):
            m, rows, parity = lax.div(t, BATCH), rows_of(t), lax.rem(t, 2)

            @pl.when(t > 0)
            def _():
                receive_rows(t, 1 - parity)
            hv = [hs1[t, x * n_x + k] for k in range(n_x)]
            for d in (1, 3, 2, 0):
                tx = lax.rem(x + d, n_x)
                for hf in range(2):
                    acc = p_f[m, tx, hf, rows] + xz_in[m, tx, hf, rows]
                    for k in range(n_x):
                        acc += jnp.dot(hv[k], w_fwd[k // 2, 2 * tx + hf, (k % 2) * chunk:(k % 2 + 1) * chunk],
                                       preferred_element_type=F32)
                    z_out[parity, tx, hf] = acc
                if d:
                    remote(z_out.at[parity, tx], z_part.at[parity, n_x - 1 - d], part_send,
                           part_sem.at[parity, n_x - 1 - d], 2 * tx, y).start()

            @pl.when(t < 3 * n_row // 2)
            def _():
                late_tile(2 * t)

            @pl.when(t == first_mid)
            def _():
                nbytes_wait(h_oth, fwd_sem)
                nbytes_wait(p_b, pb_send)
                nbytes_wait(w_two, m_sem)

            @pl.when(jnp.logical_and(t >= first_mid, jnp.logical_or(t < first_mid + 4, jnp.logical_and(t > first_mid + 4, lax.rem(t, 2) == 0))))
            def _():
                mid(jnp.where(t < first_mid + 4, 2 * (t - first_mid), lax.div(t, 2) - 1))

            for d in range(n_x - 1):
                nbytes_wait(z_part.at[parity, d], part_sem.at[parity, d])
            acc = []
            for hf in range(2):
                z = z_out[parity, x, hf] + bias[0, hf]
                for d in range(n_x - 1):
                    z = z + z_part[parity, d, hf]
                acc.append(z)
            cell(acc, hs1, t + 1)
            for k in range(n_col):
                to_y = lax.rem(y + k, n_col)

                def give():
                    remote(hs1.at[t + 1, own_j], hs1.at[t + 1, own_j], step_send, row_sem.at[parity, x],
                           2 * y, to_y).start()
                if k:
                    give()
                else:
                    pl.when(x != y)(give)

            @pl.when(t < 3 * n_row // 2)
            def _():
                late_tile(2 * t + 1)

            @pl.when(jnp.logical_and(t >= 2, t < 2 + 3 * PIECES // 2))
            def _():
                for k in range(4):
                    piece(4 * (t - 2) + k)

            @pl.when(jnp.logical_and(t >= first_mid, t < first_mid + 4))
            def _():
                mid(2 * (t - first_mid) + 1)
            nbytes_wait(z_out.at[0, pl.ds(0, n_x - 1)], part_send)
            return c
        lax.fori_loop(0, n_step, step_fwd, 0)
        receive_rows(n_step, (n_step - 1) % 2)
        mid(n_bat - 1)
        out_c[0] = c_st[0]
        co[0] = c_st[1]
        e = remote(co.at[0], out_c.at[0], end_send.at[2], end_sem.at[2], mate, y)
        e.start()
        e.wait_send()
        nbytes_wait(out_h, end_sem.at[0])
        nbytes_wait(out_c.at[pl.ds(1, 2)], end_sem.at[1])
        nbytes_wait(p_b, mid_send)
        nbytes_wait(send_a, a_send)
        nbytes_wait(send_c, c_send)
        nbytes_wait(hs1.at[pl.ds(0, n_step), pl.ds(0, n_col - 1)], step_send)

        @pl.when(x != y)
        def _():
            nbytes_wait(hs1.at[pl.ds(0, n_step), 0], step_send)

    nbytes_wait(hs1.at[0, pl.ds(0, 2 * n_row - 2)], init_send)
    nbytes_wait(hs1.at[0, pl.ds(0, 2 * n_row - 2)], init_send)
    nbytes_wait(c_all1.at[pl.ds(0, 2 * n_row - 2)], init_send)
    nbytes_wait(c_all1.at[pl.ds(0, 2 * n_row - 2)], init_send)


def solution(mesh):
    n_row = mesh.shape['row']
    n_col = mesh.shape['col']
    spec_seq = P(None, 'data', 'row')
    spec_weight = P(None, 'row', 'col')
    spec_out = P(None, 'data', ('col', 'row'))

    def local(x_rows, w_x1, w_h1, b_1, w_x2, w_h2, b_2, h_zero, c_zero):
        n_step, batch, deep = x_rows.shape
        cols = w_h2.shape[1]
        wide = cols // n_row
        unit = wide // 4
        n_chunk = n_row // 2 * n_col
        chunk = 2 * unit
        n_bat = n_step // BATCH
        n_x = n_row // 2

        vmem = pl.BlockSpec(memory_space=pltpu.VMEM)
        hbm = pl.BlockSpec(memory_space=pl.ANY)
        dma = pltpu.SemaphoreType.DMA
        rows = BATCH * PAD
        weights = (n_row, 2, deep, wide)
        h_out, c_out = pl.pallas_call(
            functools.partial(kernel, n_row, n_col),
            out_shape=(jax.ShapeDtypeStruct((n_step, PAD, unit), BF16),
                       jax.ShapeDtypeStruct((3, PAD, unit), F32)),
            in_specs=[vmem] * 5 + [hbm] * 4,
            out_specs=(vmem, vmem),
            scratch_shapes=[
                pltpu.VMEM((n_step * PAD, deep), BF16),
                pltpu.VMEM((3, 2, PAD, chunk), BF16),
                pltpu.VMEM((3, 2, PAD, chunk), F32),
                pltpu.VMEM((2, 2, PAD, wide), F32),
                pltpu.VMEM(weights, BF16),
                pltpu.VMEM(weights, BF16),
                pltpu.VMEM((2, n_row, deep, wide), BF16),
                pltpu.VMEM((2, n_row, deep, wide), BF16),
                pltpu.VMEM((n_row, deep, wide), BF16),
                pltpu.VMEM((n_row, deep, wide), BF16),
                pltpu.VMEM((STAGES, deep, wide), BF16),
                pltpu.VMEM((wide, wide), BF16),
                pltpu.VMEM((n_bat, n_x, 2, rows, wide), F32),
                pltpu.VMEM((n_bat, n_x, 2, rows, wide), F32),
                pltpu.VMEM((n_bat, n_x, 2, rows, wide), F32),
                pltpu.VMEM((n_bat, n_x, 2, rows, wide), F32),
                pltpu.VMEM((2, n_x, 2, PAD, wide), F32),
                pltpu.VMEM((2, n_x - 1, 2, PAD, wide), F32),
                pltpu.VMEM((2, rows, 2 * deep), F32),
                pltpu.VMEM((n_step + 1, n_chunk, PAD, chunk), BF16),
                pltpu.VMEM((n_step + 1, n_chunk, PAD, chunk), BF16),
                pltpu.VMEM((n_step, n_x, PAD, chunk), BF16),
                pltpu.VMEM((n_chunk, PAD, chunk), F32),
                pltpu.VMEM((n_chunk, PAD, chunk), F32),
                pltpu.VMEM((2, PAD, unit), F32),
                pltpu.VMEM((n_step, PAD, unit), BF16),
                pltpu.VMEM((3, PAD, unit), F32),
                dma((STAGES,)), dma(()), dma((n_row,)), dma((2,)),
                dma(()), dma(()), dma(()), dma(()),
                dma(()), dma(()), dma(()), dma((n_bat,)),
                dma(()), dma((n_bat,)), dma(()), dma((n_bat,)),
                dma(()), dma((2,)), dma((2,)),
                dma(()), dma((2, n_chunk)),
                dma(()), dma((2, n_x - 1)), dma((2, n_x)),
                dma(()), dma(()),
                dma((3,)), dma((3,)),
            ],
            compiler_params=pltpu.CompilerParams(collective_id=0, has_side_effects=True,
                                                 vmem_limit_bytes=67_043_328),
        )(x_rows.transpose(1, 0, 2), h_zero, c_zero, b_1, b_2.reshape(1, cols), w_x1, w_h1, w_x2, w_h2)
        return h_out[:, :batch], c_out[:, :batch]

    return jax.shard_map(local, mesh=mesh,
                         in_specs=(spec_seq, spec_weight, spec_weight, P(None, 'col'), spec_weight,
                                   P('row', 'col'), P('col'), spec_seq, spec_seq),
                         out_specs=(spec_out, spec_out), check_vma=False)
```

```python
import functools

import jax
import jax.numpy as jnp
from jax import lax
from jax.experimental import pallas as pl
from jax.experimental.pallas import tpu as pltpu
from jax.sharding import PartitionSpec as P

PAD = 8
STAGES = 4
BATCH = 2
FIRST_PIECE = 4
PIECES = 16
F32, BF16 = jnp.float32, jnp.bfloat16


def nbytes_wait(ref, sem):
    pltpu.make_async_copy(ref, ref, sem).wait()


def hop_groups(n_x, n_y):
    far = {}
    for dy in range(n_y):
        for dx in range(n_x):
            far.setdefault(min(dx, n_x - dx) + min(dy, n_y - dy), []).append((dx, dy))
    return [far[k] for k in sorted(far)]


def kernel(n_row, n_col, x_in, h_in, c_in, b1_in, b2_in, w_x1, w_h1, w_x2, w_h2, out_h, out_c,
           x_ref, h0_ref, c0_ref, bias, w_one, w_two, w_fwd, w_mid, send_a, send_c, stage, sort, p_b, p_f, xz_in, z_in, z_out, z_part, lhs,
           hs1, hs2, h_oth, c_all1, c_all2, c_st, ho, co,
           stage_sem, a_send, pass_sem, w_sem, f_send, f_sem, m_sem, c_send, c_sem, pf_send, pf_sem, pb_send, pb_sem, xz_send, xz_sem,
           mid_send, z_sem, init_send, h0_sem, c0_sem, step_send, step_sem, part_send, part_sem, row_sem,
           fwd_send, fwd_sem, end_send, end_sem):
    n_x = n_row // 2
    batch, n_step = x_in.shape[:2]
    n_bat = n_step // BATCH
    deep = w_h2.shape[0]
    wide = w_h2.shape[1] // n_row
    unit = wide // 4
    chunk = deep // 2
    r = lax.axis_index('row')
    y = lax.axis_index('col')
    core = lax.rem(r, 2)
    x = lax.div(r, 2)
    mate = r + 1 - 2 * core
    own_j = y * n_x + x

    def at(row, col):
        return {'row': row, 'col': col}

    def remote(src, dst, ssem, rsem, row, col):
        return pltpu.make_async_remote_copy(src_ref=src, dst_ref=dst, send_sem=ssem, recv_sem=rsem,
                                            device_id=at(row, col), device_id_type=pl.DeviceIdType.MESH)

    def group_of(i):
        near = jnp.logical_and(i >= 2, i < 6)
        dx = jnp.where(near, 1 + 2 * lax.rem(i, 2), jnp.where(i < 2, 2, 0))
        half = jnp.where(near, lax.div(i - 2, 2), lax.rem(i, 2))
        return lax.rem(x + dx, n_x), half

    def load(src, i, slot):
        tx, half = group_of(i)
        first = pl.multiple_of((2 * tx + half) * wide, wide)
        pltpu.make_async_copy(src.at[:, pl.ds(first, wide)], stage.at[slot], stage_sem.at[slot]).start()

    def load_late(n):
        slot, i = lax.rem(n, STAGES), lax.rem(n, n_row)

        @pl.when(n < n_row)
        def _():
            load(w_h2, i, slot)

        @pl.when(jnp.logical_and(n >= n_row, n < 3 * n_row))
        def _():
            load(w_x2.at[lax.div(n - n_row, n_row)], i, slot)

    def sorted_tile(slot):
        return jnp.dot(stage[slot], sort[...], preferred_element_type=F32).astype(BF16)

    def use_back(i, tile):
        tx, half = group_of(i)
        g = 2 * tx + half

        @pl.when(jnp.logical_and(tx == x, core == 1))
        def _():
            w_one[r, half] = tile

        @pl.when(jnp.logical_or(tx != x, core == 0))
        def _():
            send_a[g] = tile

        @pl.when(jnp.logical_and(tx != x, core == 1))
        def _():
            remote(send_a.at[g], w_one.at[r, half], a_send, w_sem.at[0], 2 * tx + 1, y).start()

        @pl.when(jnp.logical_and(tx != x, core == 0))
        def _():
            remote(send_a.at[g], w_fwd.at[1, g], a_send, pass_sem.at[i], mate, y).start()

        @pl.when(jnp.logical_and(tx == x, core == 0))
        def _():
            remote(send_a.at[g], w_one.at[r, half], a_send, w_sem.at[0], mate, y).start()

    def pass_back(i, c):
        tx, half = group_of(i)
        g = 2 * tx + half
        nbytes_wait(w_fwd.at[1, g], pass_sem.at[i])
        remote(w_fwd.at[1, g], w_one.at[mate, half], a_send, w_sem.at[0], 2 * tx + 1, y).start()
        return c

    def use_fwd(i, tile):
        tx, half = group_of(i)
        g = 2 * tx + half
        w_fwd[0, g] = tile

        @pl.when(core == 1)
        def _():
            remote(w_fwd.at[0, g], w_fwd.at[1, g], f_send, f_sem, mate, y).start()

    def project(buf):
        def use(i, tile):
            tx, half = group_of(i)
            z = jnp.dot(x_ref[...], tile, preferred_element_type=F32)
            for m in range(n_bat):
                buf[m, tx, half] = z[m * BATCH * PAD:(m + 1) * BATCH * PAD]
        return use

    def late_tile(n):
        slot = lax.rem(n, STAGES)
        nbytes_wait(stage.at[slot], stage_sem.at[slot])
        load_late(n + STAGES - 1)
        tile = sorted_tile(slot)
        tx, half = group_of(lax.rem(n, n_row))
        g = 2 * tx + half

        @pl.when(n >= n_row)
        def _():
            k = lax.div(n - n_row, n_row)
            w_mid[k, g] = tile

            @pl.when(core == 1)
            def _():
                remote(w_mid.at[k, g], w_two.at[g, k], f_send, m_sem, mate, y).start()

        @pl.when(jnp.logical_and(n < n_row, jnp.logical_and(tx == x, core == 1)))
        def _():
            w_two[r, half] = tile

        @pl.when(jnp.logical_and(n < n_row, jnp.logical_or(tx != x, core == 0)))
        def _():
            send_c[g] = tile

        @pl.when(jnp.logical_and(n < n_row, jnp.logical_and(tx == x, core == 0)))
        def _():
            remote(send_c.at[g], w_two.at[r, half], c_send, w_sem.at[1], mate, y).start()

        @pl.when(jnp.logical_and(n < n_row, jnp.logical_and(tx != x, core == 1)))
        def _():
            remote(send_c.at[g], w_one.at[tx, half], c_send, c_sem, mate, y).start()

    def pieces(p):
        half, q = lax.div(p, 3 * PIECES), lax.rem(p, 3 * PIECES)
        k, e = lax.div(q, 3), lax.rem(q, 3)
        tx = lax.rem(x + jnp.where(e < 2, 1 + 2 * e, 2), n_x)
        n_rows = deep // PIECES
        rows = pl.ds(pl.multiple_of(k * n_rows, n_rows), n_rows)
        for src, owner in ((send_c.at[2 * tx + half, rows], r), (w_one.at[tx, half, rows], mate)):
            remote(src, w_two.at[owner, half, rows], c_send, w_sem.at[1], 2 * tx + 1, y).start()

    jobs = [(w_h1.at[1], use_back), (w_h1.at[0], use_fwd), (w_x1.at[0], project(p_f)), (w_x1.at[1], project(p_b))]
    for i in range(STAGES - 1):
        load(jobs[0][0], i, i)
    barrier = pltpu.get_barrier_semaphore()

    def greet():
        for dc in range(n_col):
            for dr in range(n_row):
                if dc or dr:
                    pl.semaphore_signal(barrier, inc=1, device_id=at(lax.rem(r + dr, n_row), lax.rem(y + dc, n_col)),
                                        device_id_type=pl.DeviceIdType.MESH)

    def iota2(shape):
        return lax.broadcasted_iota(jnp.int32, shape, 0), lax.broadcasted_iota(jnp.int32, shape, 1)

    def make_sort():
        rows_i, cols_i = iota2((wide, wide))
        gate_i, unit_i = lax.div(cols_i, unit), lax.rem(cols_i, unit)
        sort[...] = jnp.where(rows_i == 4 * unit_i + gate_i, 1.0, 0.0).astype(BF16)

    def pad_states():
        for k in range(3):
            lhs[0, 0:PAD, 0:deep] = jnp.zeros((PAD, deep), F32)
            lhs[0, 0:batch, 0:deep] = h_in[k]
            for jj in range(2):
                here = slice(jj * chunk, (jj + 1) * chunk)
                h0_ref[k, jj] = lhs[0, 0:PAD, here].astype(BF16)
                c0_ref[k, jj] = jnp.zeros((PAD, chunk), F32)
                c0_ref[k, jj, 0:batch] = c_in[k, :, here]

    greet()
    make_sort()
    pad_states()
    pl.semaphore_wait(barrier, n_col * n_row - 1)

    def share_states():
        for d in range(1, n_row):
            to = lax.rem(r + d, n_row)
            tc = lax.rem(to, 2)
            here = pl.ds(2 * r, 2)
            remote(h0_ref.at[tc], hs1.at[tc * n_step, here], init_send, h0_sem.at[0], to, y).start()
            remote(h0_ref.at[2], hs2.at[0, here], init_send, h0_sem.at[1], to, y).start()
            remote(c0_ref.at[tc], c_all1.at[here], init_send, c0_sem.at[0], to, y).start()
            remote(c0_ref.at[2], c_all2.at[here], init_send, c0_sem.at[1], to, y).start()
        hs1[core * n_step, pl.ds(2 * r, 2)] = h0_ref[core]
        hs2[0, pl.ds(2 * r, 2)] = h0_ref[2]
        c_all1[pl.ds(2 * r, 2)] = c0_ref[core]
        c_all2[pl.ds(2 * r, 2)] = c0_ref[2]

    share_states()

    def prepare():
        for hf in range(2):
            cols = pl.ds(pl.multiple_of((2 * x + hf) * wide, wide), wide)
            for n, b_row in enumerate((b1_in[pl.ds(core, 1), cols], b2_in[:, cols])):
                left = jnp.broadcast_to(b_row * 0.5, (PAD, wide))
                total = jnp.zeros((PAD, wide), F32)
                for _ in range(3):
                    part = left.astype(BF16)
                    total += jnp.dot(part, sort[...], preferred_element_type=F32)
                    left = left - part.astype(F32)
                bias[n, hf] = total * 2.0

        rows_i, cols_i = iota2((n_step * PAD, batch * n_step))
        take = jnp.where(cols_i == lax.rem(rows_i, PAD) * n_step + lax.div(rows_i, PAD), 1.0, 0.0)
        take = jnp.where(lax.rem(rows_i, PAD) < batch, take, 0.0).astype(BF16)
        flat = x_in[...].astype(F32).reshape(batch * n_step, deep).astype(BF16)
        x_ref[...] = jnp.dot(take, flat, preferred_element_type=F32).astype(BF16)

    for n, (src, use) in enumerate(jobs):
        def body(i, c):
            slot = lax.rem(i, STAGES)
            nbytes_wait(stage.at[slot], stage_sem.at[slot])
            ahead = i + STAGES - 1
            slot_ahead = lax.rem(ahead, STAGES)

            @pl.when(ahead < n_row)
            def _():
                load(src, ahead, slot_ahead)

            @pl.when(ahead >= n_row)
            def _():
                load(jobs[n + 1][0] if n + 1 < len(jobs) else w_h2, ahead - n_row, slot_ahead)
            use(i, sorted_tile(slot))
            return c
        lax.fori_loop(0, n_row, body, 0)
        if n == 0:
            @pl.when(core == 1)
            def _():
                lax.fori_loop(0, n_row - 2, pass_back, 0)
            prepare()
        if n == 2:
            @pl.when(core == 1)
            def _():
                remote(p_f, xz_in, pf_send, pf_sem, mate, y).start()

    nbytes_wait(hs1.at[0, pl.ds(0, 2 * n_row - 2)], h0_sem.at[0])
    nbytes_wait(hs2.at[0, pl.ds(0, 2 * n_row - 2)], h0_sem.at[1])
    nbytes_wait(c_all1.at[pl.ds(0, 2 * n_row - 2)], c0_sem.at[0])
    nbytes_wait(c_all2.at[pl.ds(0, 2 * n_row - 2)], c0_sem.at[1])

    def own_state(c_all):
        for hf in range(2):
            c_st[hf] = c_all[own_j, :, hf * unit:(hf + 1) * unit]
    own_state(c_all1)

    def rows_of(t):
        return pl.ds(pl.multiple_of(lax.rem(t, BATCH) * PAD, PAD), PAD)

    def cell(acc, hs, new):
        h_new = []
        for hf in range(2):
            gate = [acc[hf][:, k * unit:(k + 1) * unit] for k in range(4)]
            c = (jax.nn.sigmoid(gate[1]) * c_st[hf]
                 + jax.nn.sigmoid(gate[0]) * jnp.tanh(gate[2]))
            c_st[hf] = c
            h = (jax.nn.sigmoid(gate[3]) * jnp.tanh(c)).astype(BF16)
            hs[new, own_j, :, hf * unit:(hf + 1) * unit] = h
            h_new.append(h)
        return h_new

    def to_mate(slot):
        return remote(hs1.at[slot, pl.ds(x * n_x, n_x)], h_oth.at[slot], fwd_send, fwd_sem, mate, y)

    def mid(m, parts=(0, 1), after=False):
        for i in range(BATCH):
            for jj in range(n_x):
                here = slice(i * PAD, (i + 1) * PAD), slice(jj * chunk, (jj + 1) * chunk)
                if 0 in parts:
                    lhs[0, here[0], here[1]] = hs1[m * BATCH + i + 1, x * n_x + jj].astype(F32)
                if 1 in parts:
                    lhs[1, here[0], here[1]] = h_oth[m * BATCH + i, jj].astype(F32)
        left = {k: [lhs[k, :, c * deep:(c + 1) * deep].astype(BF16) for c in range(2)] for k in parts}

        def one(i, c):
            d = jnp.where(i == n_x - 1, 0, jnp.where(i == 0, 2, 2 * i - 1))
            tx = lax.rem(x + d, n_x)
            for hf in range(2):
                g = 2 * tx + hf
                z = p_b[m, tx, hf] if after else jnp.zeros((BATCH * PAD, wide), F32)
                for k in parts:
                    z += jnp.dot(left[k][0], w_mid[k, g], preferred_element_type=F32)
                    z += jnp.dot(left[k][1], w_two[g, k], preferred_element_type=F32)
                p_b[m, tx, hf] = z
            if 1 in parts:
                remote(p_b.at[m, tx], z_in.at[m, lax.rem(n_x - d, n_x)], mid_send, z_sem.at[m], 2 * tx + 1, y).start()
            return c
        lax.fori_loop(0, n_x, one, 0)

    sends = [o for grp in hop_groups(n_x, n_col) for o in grp][:0:-1]

    def along(pos, n):
        inner = lax.rem(1 - 2 * lax.rem(pos, 2) + n, n)
        return {'0': 0, 'I': inner, 'O': n - inner, 'F': n // 2}
    dxs, dys = along(x, n_x), along(y, n_col)
    groups = [g.split() for g in ('00', 'I0 0I', 'II O0 0O', 'F0 0F IO OI', 'OO FI IF', 'FO OF', 'FF')]

    def source(name):
        dx, dy = dxs[name[0]], dys[name[1]]
        return lax.rem(y + dy, n_col) * n_x + lax.rem(x + dx, n_x), dy * n_x + dx

    def chain_step(hs, w, prev, new, s, z_of, layer, first, last_send, after_receive):
        parity = lax.rem(s, 2)
        acc = [z_of(hf) + bias[layer, hf] for hf in range(2)]
        for n, grp in enumerate(groups):
            if n and not first:
                for name in grp:
                    j, i = source(name)
                    nbytes_wait(hs.at[prev, j], step_sem.at[1 - parity, i])
            if n == len(groups) - 1 and not first:
                after_receive()
            for name in grp:
                j, _ = source(name)
                h = hs[prev, j]
                rows = pl.ds(pl.multiple_of(lax.rem(j, 2) * chunk, chunk), chunk)
                for hf in range(2):
                    acc[hf] += jnp.dot(h, w[lax.div(j, 2), hf, rows], preferred_element_type=F32)
        h_new = cell(acc, hs, new)

        def send():
            for dx, dy in sends:
                remote(hs.at[new, own_j], hs.at[new, own_j], step_send,
                       step_sem.at[parity, (n_col - dy) % n_col * n_x + (n_x - dx) % n_x],
                       2 * lax.rem(x + dx, n_x) + 1, lax.rem(y + dy, n_col)).start()
        if last_send:
            send()
        else:
            pl.when(s < n_step - 1)(send)
        return h_new

    @pl.when(core == 1)
    def _():
        for m in reversed(range(n_bat)):
            remote(p_b.at[m], z_in.at[m], pb_send, pb_sem.at[m], mate, y).start()

        def tiles(n, c):
            late_tile(n)
            return c
        lax.fori_loop(0, 3 * n_row, tiles, 0)
        nbytes_wait(w_one.at[pl.ds(0, n_row - 1)], w_sem.at[0])

        def step_one(s, c, first=False):
            t = n_step - 1 - s
            m, rows = lax.div(t, BATCH), rows_of(t)

            @pl.when(lax.rem(s, BATCH) == 0)
            def _():
                nbytes_wait(xz_in.at[m], xz_sem.at[m])

            def z_of(hf):
                z = xz_in[m, 0, hf, rows]
                for d in range(1, n_x):
                    z = z + xz_in[m, d, hf, rows]
                return z

            chain_step(hs1, w_one, t + 1, t, s, z_of, 0, first, True, lambda: to_mate(t + 1).start())
            return c
        step_one(jnp.int32(0), 0, True)
        lax.fori_loop(1, n_step, step_one, 0)
        for grp in groups[1:]:
            for name in grp:
                j, i = source(name)
                nbytes_wait(hs1.at[0, j], step_sem.at[(n_step - 1) % 2, i])
        to_mate(0).start()
        co[1] = c_st[0]
        out_c[1] = c_st[1]
        own_state(c_all2)
        nbytes_wait(w_two.at[pl.ds(0, n_row - 1)], w_sem.at[1])

        def step_two(t, c, first=False):
            m, rows = lax.div(t, BATCH), rows_of(t)

            @pl.when(lax.rem(t, BATCH) == 0)
            def _():
                nbytes_wait(z_in.at[m], z_sem.at[m])

            def z_of(hf):
                z = z_in[m, 0, hf, rows]
                for d in range(1, n_x):
                    z = z + z_in[m, d, hf, rows]
                return z
            h_new = chain_step(hs2, w_two, t, t + 1, t, z_of, 1, first, False, lambda: None)
            ho[t] = h_new[0]
            out_h[t] = h_new[1]
            return c
        step_two(jnp.int32(0), 0, True)
        lax.fori_loop(1, n_step, step_two, 0)
        co[2] = c_st[0]
        out_c[2] = c_st[1]
        ends = [remote(ho, out_h, end_send.at[0], end_sem.at[0], mate, y),
                remote(co.at[pl.ds(1, 2)], out_c.at[pl.ds(1, 2)], end_send.at[1], end_sem.at[1], mate, y)]
        for e in ends:
            e.start()
        for e in ends:
            e.wait_send()
        nbytes_wait(out_c.at[0], end_sem.at[2])
        nbytes_wait(hs1.at[pl.ds(0, n_step), pl.ds(0, n_x * n_col - 1)], step_send)
        nbytes_wait(hs2.at[pl.ds(0, n_step - 1), pl.ds(0, n_x * n_col - 1)], step_send)
        nbytes_wait(p_b, pb_send)
        nbytes_wait(h_oth, fwd_send)
        nbytes_wait(p_f, pf_send)
        nbytes_wait(w_fwd.at[0], f_send)
        nbytes_wait(w_mid, f_send)
        nbytes_wait(send_a.at[pl.ds(0, n_row - 2)], a_send)
        nbytes_wait(send_a.at[pl.ds(0, n_row - 2)], a_send)
        nbytes_wait(send_c.at[pl.ds(0, n_row - 2)], c_send)

    @pl.when(core == 0)
    def _():
        def send_batch(m):
            nbytes_wait(z_in.at[m], pb_sem.at[m])
            for d in (2, 1, 3, 0):
                tx = lax.rem(x + d, n_x)
                p_b[m, tx] += z_in[m, tx]
                remote(p_b.at[m, tx], xz_in.at[m, (n_x - d) % n_x], xz_send, xz_sem.at[m], 2 * tx + 1, y).start()
        send_batch(n_bat - 1)
        send_batch(n_bat - 2)
        nbytes_wait(xz_in, pf_sem)
        nbytes_wait(w_fwd.at[1], f_sem)
        first_mid = n_step - 11

        def receive_rows(slot, parity):
            for k in range(n_x):
                @pl.when(jnp.logical_or(x != k, x != y))
                def _():
                    nbytes_wait(hs1.at[slot, x * n_x + k], row_sem.at[parity, k])

        def step_fwd(t, c):
            m, rows, parity = lax.div(t, BATCH), rows_of(t), lax.rem(t, 2)

            @pl.when(t > 0)
            def _():
                receive_rows(t, 1 - parity)
            hv = [hs1[t, x * n_x + k] for k in range(n_x)]
            for d in (1, 3, 2, 0):
                tx = lax.rem(x + d, n_x)
                for hf in range(2):
                    acc = p_f[m, tx, hf, rows] + xz_in[m, tx, hf, rows]
                    for k in range(n_x):
                        acc += jnp.dot(hv[k], w_fwd[k // 2, 2 * tx + hf, (k % 2) * chunk:(k % 2 + 1) * chunk],
                                       preferred_element_type=F32)
                    z_out[parity, tx, hf] = acc
                if d:
                    remote(z_out.at[parity, tx], z_part.at[parity, n_x - 1 - d], part_send,
                           part_sem.at[parity, n_x - 1 - d], 2 * tx, y).start()

            def share(k):
                @pl.when(t < 3 * n_row // 4)
                def _():
                    late_tile(4 * t + 2 * k)
                    late_tile(4 * t + 2 * k + 1)

                for p in range(6 - 2 * k):
                    nth = 10 * (t - FIRST_PIECE) + 6 * k + p

                    @pl.when(jnp.logical_and(t >= FIRST_PIECE, nth < 6 * PIECES))
                    def _():
                        pieces(nth)

            @pl.when(t == FIRST_PIECE)
            def _():
                nbytes_wait(w_one.at[pl.ds(0, n_x - 1)], c_sem)
            share(0)

            @pl.when(t == first_mid)
            def _():
                nbytes_wait(p_b, xz_send)
                nbytes_wait(w_two, m_sem)
                mid(0, (0,))
                nbytes_wait(h_oth, fwd_sem)
                mid(0, (1,), True)

            @pl.when(jnp.logical_and(t > first_mid, jnp.logical_or(t < first_mid + 4, jnp.logical_and(t > first_mid + 4, lax.rem(t, 2) == 0))))
            def _():
                mid(jnp.where(t < first_mid + 4, 2 * (t - first_mid), lax.div(t, 2) - 1))

            for d in range(n_x - 1):
                nbytes_wait(z_part.at[parity, d], part_sem.at[parity, d])
            acc = []
            for hf in range(2):
                z = z_out[parity, x, hf] + bias[0, hf]
                for d in range(n_x - 1):
                    z = z + z_part[parity, d, hf]
                acc.append(z)
            cell(acc, hs1, t + 1)
            for k in range(n_col):
                to_y = lax.rem(y + k, n_col)

                def give():
                    remote(hs1.at[t + 1, own_j], hs1.at[t + 1, own_j], step_send, row_sem.at[parity, x],
                           2 * y, to_y).start()
                if k:
                    give()
                else:
                    pl.when(x != y)(give)

            share(1)

            @pl.when(jnp.logical_and(t >= 2, t < n_bat))
            def _():
                send_batch(n_bat - 1 - t)

            @pl.when(jnp.logical_and(t >= first_mid, t < first_mid + 4))
            def _():
                mid(2 * (t - first_mid) + 1)
            nbytes_wait(z_out.at[0, pl.ds(0, n_x - 1)], part_send)
            return c
        lax.fori_loop(0, n_step, step_fwd, 0)
        receive_rows(n_step, (n_step - 1) % 2)
        mid(n_bat - 1)
        out_c[0] = c_st[0]
        co[0] = c_st[1]
        e = remote(co.at[0], out_c.at[0], end_send.at[2], end_sem.at[2], mate, y)
        e.start()
        e.wait_send()
        nbytes_wait(out_h, end_sem.at[0])
        nbytes_wait(out_c.at[pl.ds(1, 2)], end_sem.at[1])
        nbytes_wait(p_b, mid_send)
        nbytes_wait(send_a, a_send)
        nbytes_wait(send_c, c_send)
        nbytes_wait(send_c.at[pl.ds(0, n_row - 2)], c_send)
        nbytes_wait(hs1.at[pl.ds(0, n_step), pl.ds(0, n_col - 1)], step_send)

        @pl.when(x != y)
        def _():
            nbytes_wait(hs1.at[pl.ds(0, n_step), 0], step_send)

    nbytes_wait(hs1.at[0, pl.ds(0, 2 * n_row - 2)], init_send)
    nbytes_wait(hs1.at[0, pl.ds(0, 2 * n_row - 2)], init_send)
    nbytes_wait(c_all1.at[pl.ds(0, 2 * n_row - 2)], init_send)
    nbytes_wait(c_all1.at[pl.ds(0, 2 * n_row - 2)], init_send)


def solution(mesh):
    n_row = mesh.shape['row']
    n_col = mesh.shape['col']
    spec_seq = P(None, 'data', 'row')
    spec_weight = P(None, 'row', 'col')
    spec_out = P(None, 'data', ('col', 'row'))

    def local(x_rows, w_x1, w_h1, b_1, w_x2, w_h2, b_2, h_zero, c_zero):
        n_step, batch, deep = x_rows.shape
        cols = w_h2.shape[1]
        wide = cols // n_row
        unit = wide // 4
        n_chunk = n_row // 2 * n_col
        chunk = 2 * unit
        n_bat = n_step // BATCH
        n_x = n_row // 2

        vmem = pl.BlockSpec(memory_space=pltpu.VMEM)
        hbm = pl.BlockSpec(memory_space=pl.ANY)
        dma = pltpu.SemaphoreType.DMA
        rows = BATCH * PAD
        weights = (n_row, 2, deep, wide)
        h_out, c_out = pl.pallas_call(
            functools.partial(kernel, n_row, n_col),
            out_shape=(jax.ShapeDtypeStruct((n_step, PAD, unit), BF16),
                       jax.ShapeDtypeStruct((3, PAD, unit), F32)),
            in_specs=[vmem] * 5 + [hbm] * 4,
            out_specs=(vmem, vmem),
            scratch_shapes=[
                pltpu.VMEM((n_step * PAD, deep), BF16),
                pltpu.VMEM((3, 2, PAD, chunk), BF16),
                pltpu.VMEM((3, 2, PAD, chunk), F32),
                pltpu.VMEM((2, 2, PAD, wide), F32),
                pltpu.VMEM(weights, BF16),
                pltpu.VMEM(weights, BF16),
                pltpu.VMEM((2, n_row, deep, wide), BF16),
                pltpu.VMEM((2, n_row, deep, wide), BF16),
                pltpu.VMEM((n_row, deep, wide), BF16),
                pltpu.VMEM((n_row, deep, wide), BF16),
                pltpu.VMEM((STAGES, deep, wide), BF16),
                pltpu.VMEM((wide, wide), BF16),
                pltpu.VMEM((n_bat, n_x, 2, rows, wide), F32),
                pltpu.VMEM((n_bat, n_x, 2, rows, wide), F32),
                pltpu.VMEM((n_bat, n_x, 2, rows, wide), F32),
                pltpu.VMEM((n_bat, n_x, 2, rows, wide), F32),
                pltpu.VMEM((2, n_x, 2, PAD, wide), F32),
                pltpu.VMEM((2, n_x - 1, 2, PAD, wide), F32),
                pltpu.VMEM((2, rows, 2 * deep), F32),
                pltpu.VMEM((n_step + 1, n_chunk, PAD, chunk), BF16),
                pltpu.VMEM((n_step + 1, n_chunk, PAD, chunk), BF16),
                pltpu.VMEM((n_step, n_x, PAD, chunk), BF16),
                pltpu.VMEM((n_chunk, PAD, chunk), F32),
                pltpu.VMEM((n_chunk, PAD, chunk), F32),
                pltpu.VMEM((2, PAD, unit), F32),
                pltpu.VMEM((n_step, PAD, unit), BF16),
                pltpu.VMEM((3, PAD, unit), F32),
                dma((STAGES,)), dma(()), dma((n_row,)), dma((2,)),
                dma(()), dma(()), dma(()), dma(()), dma(()),
                dma(()), dma(()), dma(()), dma((n_bat,)),
                dma(()), dma((n_bat,)), dma(()), dma((n_bat,)),
                dma(()), dma((2,)), dma((2,)),
                dma(()), dma((2, n_chunk)),
                dma(()), dma((2, n_x - 1)), dma((2, n_x)),
                dma(()), dma(()),
                dma((3,)), dma((3,)),
            ],
            compiler_params=pltpu.CompilerParams(collective_id=0, has_side_effects=True,
                                                 vmem_limit_bytes=67_043_328),
        )(x_rows.transpose(1, 0, 2), h_zero, c_zero, b_1, b_2.reshape(1, cols), w_x1, w_h1, w_x2, w_h2)
        return h_out[:, :batch], c_out[:, :batch]

    return jax.shard_map(local, mesh=mesh,
                         in_specs=(spec_seq, spec_weight, spec_weight, P(None, 'col'), spec_weight,
                                   P('row', 'col'), P('col'), spec_seq, spec_seq),
                         out_specs=(spec_out, spec_out), check_vma=False)
```

```python
import functools

import jax
import jax.numpy as jnp
from jax import lax
from jax.experimental import pallas as pl
from jax.experimental.pallas import tpu as pltpu
from jax.sharding import PartitionSpec as P

PAD = 8
STAGES = 4
BATCH = 2
FIRST_PIECE = 4
PIECES = 32
F32, BF16 = jnp.float32, jnp.bfloat16


def nbytes_wait(ref, sem):
    pltpu.make_async_copy(ref, ref, sem).wait()


def hop_groups(n_x, n_y):
    far = {}
    for dy in range(n_y):
        for dx in range(n_x):
            far.setdefault(min(dx, n_x - dx) + min(dy, n_y - dy), []).append((dx, dy))
    return [far[k] for k in sorted(far)]


def kernel(n_row, n_col, x_in, h_in, c_in, b1_in, b2_in, w_x1, w_h1, w_x2, w_h2, out_h, out_c,
           x_ref, h0_ref, c0_ref, bias, z_first, w_one, w_two, w_fwd, w_mid, send_a, send_c, stage, sort, p_b, p_f, xz_in, z_in, z_out, z_part, lhs,
           hs1, hs2, h_oth, c_all1, c_all2, c_st, ho, co,
           stage_sem, a_send, pass_sem, w_sem, f_send, f_sem, m_sem, c_send, c_sem, pf_send, pf_sem, pb_send, pb_sem, xz_send, xz_sem,
           mid_send, z_sem, init_send, h0_sem, c0_sem, step_send, step_sem, part_send, part_sem, row_sem,
           fwd_send, fwd_sem, end_send, end_sem):
    n_x = n_row // 2
    batch, n_step = x_in.shape[:2]
    n_bat = n_step // BATCH
    deep = w_h2.shape[0]
    wide = w_h2.shape[1] // n_row
    unit = wide // 4
    chunk = deep // 2
    r = lax.axis_index('row')
    y = lax.axis_index('col')
    core = lax.rem(r, 2)
    x = lax.div(r, 2)
    mate = r + 1 - 2 * core
    own_j = y * n_x + x

    def at(row, col):
        return {'row': row, 'col': col}

    def remote(src, dst, ssem, rsem, row, col):
        return pltpu.make_async_remote_copy(src_ref=src, dst_ref=dst, send_sem=ssem, recv_sem=rsem,
                                            device_id=at(row, col), device_id_type=pl.DeviceIdType.MESH)

    def group_of(i):
        near = jnp.logical_and(i >= 2, i < 6)
        dx = jnp.where(near, 1 + 2 * lax.rem(i, 2), jnp.where(i < 2, 2, 0))
        half = jnp.where(near, lax.div(i - 2, 2), lax.rem(i, 2))
        return lax.rem(x + dx, n_x), half

    def load(src, i, slot):
        tx, half = group_of(i)
        first = pl.multiple_of((2 * tx + half) * wide, wide)
        pltpu.make_async_copy(src.at[:, pl.ds(first, wide)], stage.at[slot], stage_sem.at[slot]).start()

    def load_late(n):
        slot, i = lax.rem(n, STAGES), lax.rem(n, n_row)

        @pl.when(n < n_row)
        def _():
            load(w_h2, i, slot)

        @pl.when(jnp.logical_and(n >= n_row, n < 3 * n_row))
        def _():
            load(w_x2.at[lax.div(n - n_row, n_row)], i, slot)

    def sorted_tile(slot):
        return jnp.dot(stage[slot], sort[...], preferred_element_type=F32).astype(BF16)

    def use_back(i, tile):
        tx, half = group_of(i)
        g = 2 * tx + half
        z_first[tx, half] = (jnp.dot(h0_ref[1, 0], tile[:chunk], preferred_element_type=F32)
                             + jnp.dot(h0_ref[1, 1], tile[chunk:], preferred_element_type=F32))

        @pl.when(jnp.logical_and(tx == x, core == 1))
        def _():
            w_one[r, half] = tile

        @pl.when(jnp.logical_or(tx != x, core == 0))
        def _():
            send_a[g] = tile

        @pl.when(jnp.logical_and(tx != x, core == 1))
        def _():
            remote(send_a.at[g], w_one.at[r, half], a_send, w_sem.at[0], 2 * tx + 1, y).start()

        @pl.when(jnp.logical_and(tx != x, core == 0))
        def _():
            remote(send_a.at[g], w_fwd.at[1, g], a_send, pass_sem.at[i], mate, y).start()

        @pl.when(jnp.logical_and(tx == x, core == 0))
        def _():
            remote(send_a.at[g], w_one.at[r, half], a_send, w_sem.at[0], mate, y).start()

    def pass_back(i, c):
        tx, half = group_of(i)
        g = 2 * tx + half
        nbytes_wait(w_fwd.at[1, g], pass_sem.at[i])
        remote(w_fwd.at[1, g], w_one.at[mate, half], a_send, w_sem.at[0], 2 * tx + 1, y).start()
        return c

    def use_fwd(i, tile):
        tx, half = group_of(i)
        g = 2 * tx + half
        w_fwd[0, g] = tile

        @pl.when(core == 1)
        def _():
            remote(w_fwd.at[0, g], w_fwd.at[1, g], f_send, f_sem, mate, y).start()

    def project(buf):
        def use(i, tile):
            tx, half = group_of(i)
            z = jnp.dot(x_ref[...], tile, preferred_element_type=F32)
            for m in range(n_bat):
                buf[m, tx, half] = z[m * BATCH * PAD:(m + 1) * BATCH * PAD]
        return use

    def late_tile(n):
        slot = lax.rem(n, STAGES)
        nbytes_wait(stage.at[slot], stage_sem.at[slot])
        load_late(n + STAGES - 1)
        tile = sorted_tile(slot)
        tx, half = group_of(lax.rem(n, n_row))
        g = 2 * tx + half

        @pl.when(n >= n_row)
        def _():
            k = lax.div(n - n_row, n_row)
            w_mid[k, g] = tile

            @pl.when(core == 1)
            def _():
                remote(w_mid.at[k, g], w_two.at[g, k], f_send, m_sem, mate, y).start()

        @pl.when(jnp.logical_and(n < n_row, jnp.logical_and(tx == x, core == 1)))
        def _():
            w_two[r, half] = tile

        @pl.when(jnp.logical_and(n < n_row, jnp.logical_or(tx != x, core == 0)))
        def _():
            send_c[g] = tile

        @pl.when(jnp.logical_and(n < n_row, jnp.logical_and(tx == x, core == 0)))
        def _():
            remote(send_c.at[g], w_two.at[r, half], c_send, w_sem.at[1], mate, y).start()

        @pl.when(jnp.logical_and(n < n_row, jnp.logical_and(tx != x, core == 1)))
        def _():
            remote(send_c.at[g], w_one.at[tx, half], c_send, c_sem, mate, y).start()

    def pieces(p):
        half, q = lax.div(p, 3 * PIECES), lax.rem(p, 3 * PIECES)
        k, e = lax.div(q, 3), lax.rem(q, 3)
        tx = lax.rem(x + jnp.where(e < 2, 1 + 2 * e, 2), n_x)
        n_rows = deep // PIECES
        rows = pl.ds(pl.multiple_of(k * n_rows, n_rows), n_rows)
        for src, owner in ((send_c.at[2 * tx + half, rows], r), (w_one.at[tx, half, rows], mate)):
            remote(src, w_two.at[owner, half, rows], c_send, w_sem.at[1], 2 * tx + 1, y).start()

    jobs = [(w_h1.at[1], use_back), (w_h1.at[0], use_fwd), (w_x1.at[0], project(p_f)), (w_x1.at[1], project(p_b))]
    for i in range(STAGES - 1):
        load(jobs[0][0], i, i)
    barrier = pltpu.get_barrier_semaphore()

    def greet():
        for dc in range(n_col):
            for dr in range(n_row):
                if dc or dr:
                    pl.semaphore_signal(barrier, inc=1, device_id=at(lax.rem(r + dr, n_row), lax.rem(y + dc, n_col)),
                                        device_id_type=pl.DeviceIdType.MESH)

    def iota2(shape):
        return lax.broadcasted_iota(jnp.int32, shape, 0), lax.broadcasted_iota(jnp.int32, shape, 1)

    def make_sort():
        rows_i, cols_i = iota2((wide, wide))
        gate_i, unit_i = lax.div(cols_i, unit), lax.rem(cols_i, unit)
        sort[...] = jnp.where(rows_i == 4 * unit_i + gate_i, 1.0, 0.0).astype(BF16)

    def pad_states():
        for k in range(3):
            lhs[0, 0:PAD, 0:deep] = jnp.zeros((PAD, deep), F32)
            lhs[0, 0:batch, 0:deep] = h_in[k]
            for jj in range(2):
                here = slice(jj * chunk, (jj + 1) * chunk)
                h0_ref[k, jj] = lhs[0, 0:PAD, here].astype(BF16)
                c0_ref[k, jj] = jnp.zeros((PAD, chunk), F32)
                c0_ref[k, jj, 0:batch] = c_in[k, :, here]

    greet()
    make_sort()
    pad_states()
    pl.semaphore_wait(barrier, n_col * n_row - 1)

    def share_states():
        for d in range(1, n_row):
            to = lax.rem(r + d, n_row)
            tc = lax.rem(to, 2)
            here = pl.ds(2 * r, 2)
            remote(h0_ref.at[tc], hs1.at[tc * n_step, here], init_send, h0_sem.at[0], to, y).start()
            remote(h0_ref.at[2], hs2.at[0, here], init_send, h0_sem.at[1], to, y).start()
            remote(c0_ref.at[tc], c_all1.at[here], init_send, c0_sem.at[0], to, y).start()
            remote(c0_ref.at[2], c_all2.at[here], init_send, c0_sem.at[1], to, y).start()
        hs1[core * n_step, pl.ds(2 * r, 2)] = h0_ref[core]
        hs2[0, pl.ds(2 * r, 2)] = h0_ref[2]
        c_all1[pl.ds(2 * r, 2)] = c0_ref[core]
        c_all2[pl.ds(2 * r, 2)] = c0_ref[2]

    share_states()

    def prepare():
        for hf in range(2):
            cols = pl.ds(pl.multiple_of((2 * x + hf) * wide, wide), wide)
            for n, b_row in enumerate((b1_in[pl.ds(core, 1), cols], b2_in[:, cols])):
                left = jnp.broadcast_to(b_row * 0.5, (PAD, wide))
                total = jnp.zeros((PAD, wide), F32)
                for _ in range(3):
                    part = left.astype(BF16)
                    total += jnp.dot(part, sort[...], preferred_element_type=F32)
                    left = left - part.astype(F32)
                bias[n, hf] = total * 2.0

        rows_i, cols_i = iota2((n_step * PAD, batch * n_step))
        take = jnp.where(cols_i == lax.rem(rows_i, PAD) * n_step + lax.div(rows_i, PAD), 1.0, 0.0)
        take = jnp.where(lax.rem(rows_i, PAD) < batch, take, 0.0).astype(BF16)
        flat = x_in[...].astype(F32).reshape(batch * n_step, deep).astype(BF16)
        x_ref[...] = jnp.dot(take, flat, preferred_element_type=F32).astype(BF16)

    for n, (src, use) in enumerate(jobs):
        def body(i, c):
            slot = lax.rem(i, STAGES)
            nbytes_wait(stage.at[slot], stage_sem.at[slot])
            ahead = i + STAGES - 1
            slot_ahead = lax.rem(ahead, STAGES)

            @pl.when(ahead < n_row)
            def _():
                load(src, ahead, slot_ahead)

            @pl.when(ahead >= n_row)
            def _():
                load(jobs[n + 1][0] if n + 1 < len(jobs) else w_h2, ahead - n_row, slot_ahead)
            use(i, sorted_tile(slot))
            return c
        lax.fori_loop(0, n_row, body, 0)
        if n == 0:
            @pl.when(core == 1)
            def _():
                lax.fori_loop(0, n_row - 2, pass_back, 0)
            prepare()
        if n == 2:
            @pl.when(core == 1)
            def _():
                remote(p_f, xz_in, pf_send, pf_sem, mate, y).start()

    p_b[n_bat - 1, :, :, (BATCH - 1) * PAD:] += z_first[...]

    nbytes_wait(hs1.at[0, pl.ds(0, 2 * n_row - 2)], h0_sem.at[0])
    nbytes_wait(hs2.at[0, pl.ds(0, 2 * n_row - 2)], h0_sem.at[1])
    nbytes_wait(c_all1.at[pl.ds(0, 2 * n_row - 2)], c0_sem.at[0])
    nbytes_wait(c_all2.at[pl.ds(0, 2 * n_row - 2)], c0_sem.at[1])

    def own_state(c_all):
        for hf in range(2):
            c_st[hf] = c_all[own_j, :, hf * unit:(hf + 1) * unit]
    own_state(c_all1)

    def rows_of(t):
        return pl.ds(pl.multiple_of(lax.rem(t, BATCH) * PAD, PAD), PAD)

    def cell(acc, hs, new):
        h_new = []
        for hf in range(2):
            gate = [acc[hf][:, k * unit:(k + 1) * unit] for k in range(4)]
            c = jax.nn.sigmoid(gate[1]) * c_st[hf] + jax.nn.sigmoid(gate[0]) * jnp.tanh(gate[2])
            c_st[hf] = c
            h = (jax.nn.sigmoid(gate[3]) * jnp.tanh(c)).astype(BF16)
            hs[new, own_j, :, hf * unit:(hf + 1) * unit] = h
            h_new.append(h)
        return h_new

    def to_mate(slot):
        return remote(hs1.at[slot, pl.ds(x * n_x, n_x)], h_oth.at[slot], fwd_send, fwd_sem, mate, y)

    def mid(m, parts=(0, 1), after=False):
        for i in range(BATCH):
            for jj in range(n_x):
                here = slice(i * PAD, (i + 1) * PAD), slice(jj * chunk, (jj + 1) * chunk)
                if 0 in parts:
                    lhs[0, here[0], here[1]] = hs1[m * BATCH + i + 1, x * n_x + jj].astype(F32)
                if 1 in parts:
                    lhs[1, here[0], here[1]] = h_oth[m * BATCH + i, jj].astype(F32)
        left = {k: [lhs[k, :, c * deep:(c + 1) * deep].astype(BF16) for c in range(2)] for k in parts}

        def one(i, c):
            d = jnp.where(i == n_x - 1, 0, jnp.where(i == 0, 2, 2 * i - 1))
            tx = lax.rem(x + d, n_x)
            for hf in range(2):
                g = 2 * tx + hf
                z = p_b[m, tx, hf] if after else jnp.zeros((BATCH * PAD, wide), F32)
                for k in parts:
                    z += jnp.dot(left[k][0], w_mid[k, g], preferred_element_type=F32)
                    z += jnp.dot(left[k][1], w_two[g, k], preferred_element_type=F32)
                p_b[m, tx, hf] = z
            if 1 in parts:
                remote(p_b.at[m, tx], z_in.at[m, lax.rem(n_x - d, n_x)], mid_send, z_sem.at[m], 2 * tx + 1, y).start()
            return c
        lax.fori_loop(0, n_x, one, 0)

    sends = [o for grp in hop_groups(n_x, n_col) for o in grp][:0:-1]

    def along(pos, n):
        inner = lax.rem(1 - 2 * lax.rem(pos, 2) + n, n)
        return {'0': 0, 'I': inner, 'O': n - inner, 'F': n // 2}
    dxs, dys = along(x, n_x), along(y, n_col)
    groups = [g.split() for g in ('00', 'I0', '0I', 'II', 'O0', '0O', 'F0', '0F', 'IO OI', 'OO', 'FI IF', 'FO OF', 'FF')]

    def source(name):
        dx, dy = dxs[name[0]], dys[name[1]]
        return lax.rem(y + dy, n_col) * n_x + lax.rem(x + dx, n_x), dy * n_x + dx

    def chain_step(hs, w, prev, new, s, z_of, layer, first, last_send, after_receive):
        parity = lax.rem(s, 2)
        acc = [bias[layer, hf] if first else z_of(hf) + bias[layer, hf] for hf in range(2)]
        for n, grp in enumerate(groups):
            if first and layer == 0:
                break
            if n and not first:
                for name in grp:
                    j, i = source(name)
                    nbytes_wait(hs.at[prev, j], step_sem.at[1 - parity, i])
            if n == len(groups) - 1 and not first:
                after_receive()
            for name in grp:
                j, _ = source(name)
                h = hs[prev, j]
                rows = pl.ds(pl.multiple_of(lax.rem(j, 2) * chunk, chunk), chunk)
                for hf in range(2):
                    acc[hf] += jnp.dot(h, w[lax.div(j, 2), hf, rows], preferred_element_type=F32)
        if first:
            acc = [acc[hf] + z_of(hf) for hf in range(2)]
        h_new = cell(acc, hs, new)

        def send():
            for dx, dy in sends:
                remote(hs.at[new, own_j], hs.at[new, own_j], step_send,
                       step_sem.at[parity, (n_col - dy) % n_col * n_x + (n_x - dx) % n_x],
                       2 * lax.rem(x + dx, n_x) + 1, lax.rem(y + dy, n_col)).start()
        if last_send:
            send()
        else:
            pl.when(s < n_step - 1)(send)
        return h_new

    @pl.when(core == 1)
    def _():
        for m in reversed(range(n_bat)):
            remote(p_b.at[m], z_in.at[m], pb_send, pb_sem.at[m], mate, y).start()

        def tiles(n, c):
            late_tile(n)
            return c
        lax.fori_loop(0, 3 * n_row, tiles, 0)

        def step_one(s, c, first=False):
            t = n_step - 1 - s
            m, rows = lax.div(t, BATCH), rows_of(t)

            if not first:
                @pl.when(lax.rem(s, BATCH) == 0)
                def _():
                    nbytes_wait(xz_in.at[m], xz_sem.at[m])

            def z_of(hf):
                if first and hf == 0:
                    nbytes_wait(xz_in.at[m], xz_sem.at[m])
                z = xz_in[m, 0, hf, rows]
                for d in range(1, n_x):
                    z = z + xz_in[m, d, hf, rows]
                return z

            chain_step(hs1, w_one, t + 1, t, s, z_of, 0, first, True, lambda: to_mate(t + 1).start())
            return c
        step_one(jnp.int32(0), 0, True)
        nbytes_wait(w_one.at[pl.ds(0, n_row - 1)], w_sem.at[0])
        lax.fori_loop(1, n_step, step_one, 0)
        for grp in groups[1:]:
            for name in grp:
                j, i = source(name)
                nbytes_wait(hs1.at[0, j], step_sem.at[(n_step - 1) % 2, i])
        to_mate(0).start()
        co[1] = c_st[0]
        out_c[1] = c_st[1]
        own_state(c_all2)
        nbytes_wait(w_two.at[pl.ds(0, n_row - 1)], w_sem.at[1])

        def step_two(t, c, first=False):
            m, rows = lax.div(t, BATCH), rows_of(t)

            if not first:
                @pl.when(lax.rem(t, BATCH) == 0)
                def _():
                    nbytes_wait(z_in.at[m], z_sem.at[m])

            def z_of(hf):
                if first and hf == 0:
                    nbytes_wait(z_in.at[m], z_sem.at[m])
                z = z_in[m, 0, hf, rows]
                for d in range(1, n_x):
                    z = z + z_in[m, d, hf, rows]
                return z
            h_new = chain_step(hs2, w_two, t, t + 1, t, z_of, 1, first, False, lambda: None)
            ho[t] = h_new[0]
            out_h[t] = h_new[1]
            return c
        step_two(jnp.int32(0), 0, True)
        lax.fori_loop(1, n_step, step_two, 0)
        co[2] = c_st[0]
        out_c[2] = c_st[1]
        ends = [remote(ho, out_h, end_send.at[0], end_sem.at[0], mate, y),
                remote(co.at[pl.ds(1, 2)], out_c.at[pl.ds(1, 2)], end_send.at[1], end_sem.at[1], mate, y)]
        for e in ends:
            e.start()
        for e in ends:
            e.wait_send()
        nbytes_wait(out_c.at[0], end_sem.at[2])
        nbytes_wait(hs1.at[pl.ds(0, n_step), pl.ds(0, n_x * n_col - 1)], step_send)
        nbytes_wait(hs2.at[pl.ds(0, n_step - 1), pl.ds(0, n_x * n_col - 1)], step_send)
        nbytes_wait(p_b, pb_send)
        nbytes_wait(h_oth, fwd_send)
        nbytes_wait(p_f, pf_send)
        nbytes_wait(w_fwd.at[0], f_send)
        nbytes_wait(w_mid, f_send)
        nbytes_wait(send_a.at[pl.ds(0, n_row - 2)], a_send)
        nbytes_wait(send_a.at[pl.ds(0, n_row - 2)], a_send)
        nbytes_wait(send_c.at[pl.ds(0, n_row - 2)], c_send)

    @pl.when(core == 0)
    def _():
        def send_batch(m):
            nbytes_wait(z_in.at[m], pb_sem.at[m])
            for d in (2, 1, 3, 0):
                tx = lax.rem(x + d, n_x)
                p_b[m, tx] += z_in[m, tx]
                remote(p_b.at[m, tx], xz_in.at[m, (n_x - d) % n_x], xz_send, xz_sem.at[m], 2 * tx + 1, y).start()
        send_batch(n_bat - 1)
        send_batch(n_bat - 2)
        nbytes_wait(xz_in, pf_sem)
        nbytes_wait(w_fwd.at[1], f_sem)
        first_mid = n_step - 11

        def receive_rows(slot, parity):
            for k in range(n_x):
                @pl.when(jnp.logical_or(x != k, x != y))
                def _():
                    nbytes_wait(hs1.at[slot, x * n_x + k], row_sem.at[parity, k])

        def step_fwd(t, c):
            m, rows, parity = lax.div(t, BATCH), rows_of(t), lax.rem(t, 2)

            @pl.when(t > 0)
            def _():
                receive_rows(t, 1 - parity)
            hv = [hs1[t, x * n_x + k] for k in range(n_x)]
            for d in (1, 3, 2, 0):
                tx = lax.rem(x + d, n_x)
                for hf in range(2):
                    acc = p_f[m, tx, hf, rows] + xz_in[m, tx, hf, rows]
                    for k in range(n_x):
                        acc += jnp.dot(hv[k], w_fwd[k // 2, 2 * tx + hf, (k % 2) * chunk:(k % 2 + 1) * chunk],
                                       preferred_element_type=F32)
                    z_out[parity, tx, hf] = acc
                if d:
                    remote(z_out.at[parity, tx], z_part.at[parity, n_x - 1 - d], part_send,
                           part_sem.at[parity, n_x - 1 - d], 2 * tx, y).start()

            def share(k):
                @pl.when(t < 3 * n_row // 4)
                def _():
                    late_tile(4 * t + 2 * k)
                    late_tile(4 * t + 2 * k + 1)

                for p in range(12 - 4 * k):
                    nth = 20 * (t - FIRST_PIECE) + 12 * k + p

                    @pl.when(jnp.logical_and(t >= FIRST_PIECE, nth < 6 * PIECES))
                    def _():
                        pieces(nth)

            @pl.when(t == FIRST_PIECE)
            def _():
                nbytes_wait(w_one.at[pl.ds(0, n_x - 1)], c_sem)
            share(0)

            @pl.when(t == first_mid)
            def _():
                nbytes_wait(p_b, xz_send)
                nbytes_wait(w_two, m_sem)
                mid(0, (0,))
                nbytes_wait(h_oth, fwd_sem)
                mid(0, (1,), True)

            @pl.when(jnp.logical_and(t > first_mid, jnp.logical_or(t < first_mid + 4, jnp.logical_and(t > first_mid + 4, lax.rem(t, 2) == 0))))
            def _():
                mid(jnp.where(t < first_mid + 4, 2 * (t - first_mid), lax.div(t, 2) - 1))

            for d in range(n_x - 1):
                nbytes_wait(z_part.at[parity, d], part_sem.at[parity, d])
            acc = []
            for hf in range(2):
                z = z_out[parity, x, hf] + bias[0, hf]
                for d in range(n_x - 1):
                    z = z + z_part[parity, d, hf]
                acc.append(z)
            cell(acc, hs1, t + 1)
            for k in range(n_col):
                to_y = lax.rem(y + k, n_col)

                def give():
                    remote(hs1.at[t + 1, own_j], hs1.at[t + 1, own_j], step_send, row_sem.at[parity, x],
                           2 * y, to_y).start()
                if k:
                    give()
                else:
                    pl.when(x != y)(give)

            share(1)

            @pl.when(jnp.logical_and(t >= 1, t < n_bat - 1))
            def _():
                send_batch(n_bat - 2 - t)

            @pl.when(jnp.logical_and(t >= first_mid, t < first_mid + 4))
            def _():
                mid(2 * (t - first_mid) + 1)
            nbytes_wait(z_out.at[0, pl.ds(0, n_x - 1)], part_send)
            return c
        lax.fori_loop(0, n_step, step_fwd, 0)
        receive_rows(n_step, (n_step - 1) % 2)
        mid(n_bat - 1)
        out_c[0] = c_st[0]
        co[0] = c_st[1]
        e = remote(co.at[0], out_c.at[0], end_send.at[2], end_sem.at[2], mate, y)
        e.start()
        e.wait_send()
        nbytes_wait(out_h, end_sem.at[0])
        nbytes_wait(out_c.at[pl.ds(1, 2)], end_sem.at[1])
        nbytes_wait(p_b, mid_send)
        nbytes_wait(send_a, a_send)
        nbytes_wait(send_c, c_send)
        nbytes_wait(send_c.at[pl.ds(0, n_row - 2)], c_send)
        nbytes_wait(hs1.at[pl.ds(0, n_step), pl.ds(0, n_col - 1)], step_send)

        @pl.when(x != y)
        def _():
            nbytes_wait(hs1.at[pl.ds(0, n_step), 0], step_send)

    nbytes_wait(hs1.at[0, pl.ds(0, 2 * n_row - 2)], init_send)
    nbytes_wait(hs1.at[0, pl.ds(0, 2 * n_row - 2)], init_send)
    nbytes_wait(c_all1.at[pl.ds(0, 2 * n_row - 2)], init_send)
    nbytes_wait(c_all1.at[pl.ds(0, 2 * n_row - 2)], init_send)


def solution(mesh):
    n_row = mesh.shape['row']
    n_col = mesh.shape['col']
    spec_seq = P(None, 'data', 'row')
    spec_weight = P(None, 'row', 'col')
    spec_out = P(None, 'data', ('col', 'row'))

    def local(x_rows, w_x1, w_h1, b_1, w_x2, w_h2, b_2, h_zero, c_zero):
        n_step, batch, deep = x_rows.shape
        cols = w_h2.shape[1]
        wide = cols // n_row
        unit = wide // 4
        n_chunk = n_row // 2 * n_col
        chunk = 2 * unit
        n_bat = n_step // BATCH
        n_x = n_row // 2

        vmem = pl.BlockSpec(memory_space=pltpu.VMEM)
        hbm = pl.BlockSpec(memory_space=pl.ANY)
        dma = pltpu.SemaphoreType.DMA
        rows = BATCH * PAD
        weights = (n_row, 2, deep, wide)
        h_out, c_out = pl.pallas_call(
            functools.partial(kernel, n_row, n_col),
            out_shape=(jax.ShapeDtypeStruct((n_step, PAD, unit), BF16),
                       jax.ShapeDtypeStruct((3, PAD, unit), F32)),
            in_specs=[vmem] * 5 + [hbm] * 4,
            out_specs=(vmem, vmem),
            scratch_shapes=[
                pltpu.VMEM((n_step * PAD, deep), BF16),
                pltpu.VMEM((3, 2, PAD, chunk), BF16),
                pltpu.VMEM((3, 2, PAD, chunk), F32),
                pltpu.VMEM((2, 2, PAD, wide), F32),
                pltpu.VMEM((n_x, 2, PAD, wide), F32),
                pltpu.VMEM(weights, BF16),
                pltpu.VMEM(weights, BF16),
                pltpu.VMEM((2, n_row, deep, wide), BF16),
                pltpu.VMEM((2, n_row, deep, wide), BF16),
                pltpu.VMEM((n_row, deep, wide), BF16),
                pltpu.VMEM((n_row, deep, wide), BF16),
                pltpu.VMEM((STAGES, deep, wide), BF16),
                pltpu.VMEM((wide, wide), BF16),
                pltpu.VMEM((n_bat, n_x, 2, rows, wide), F32),
                pltpu.VMEM((n_bat, n_x, 2, rows, wide), F32),
                pltpu.VMEM((n_bat, n_x, 2, rows, wide), F32),
                pltpu.VMEM((n_bat, n_x, 2, rows, wide), F32),
                pltpu.VMEM((2, n_x, 2, PAD, wide), F32),
                pltpu.VMEM((2, n_x - 1, 2, PAD, wide), F32),
                pltpu.VMEM((2, rows, 2 * deep), F32),
                pltpu.VMEM((n_step + 1, n_chunk, PAD, chunk), BF16),
                pltpu.VMEM((n_step + 1, n_chunk, PAD, chunk), BF16),
                pltpu.VMEM((n_step, n_x, PAD, chunk), BF16),
                pltpu.VMEM((n_chunk, PAD, chunk), F32),
                pltpu.VMEM((n_chunk, PAD, chunk), F32),
                pltpu.VMEM((2, PAD, unit), F32),
                pltpu.VMEM((n_step, PAD, unit), BF16),
                pltpu.VMEM((3, PAD, unit), F32),
                dma((STAGES,)), dma(()), dma((n_row,)), dma((2,)),
                dma(()), dma(()), dma(()), dma(()), dma(()),
                dma(()), dma(()), dma(()), dma((n_bat,)),
                dma(()), dma((n_bat,)), dma(()), dma((n_bat,)),
                dma(()), dma((2,)), dma((2,)),
                dma(()), dma((2, n_chunk)),
                dma(()), dma((2, n_x - 1)), dma((2, n_x)),
                dma(()), dma(()),
                dma((3,)), dma((3,)),
            ],
            compiler_params=pltpu.CompilerParams(collective_id=0, has_side_effects=True,
                                                 vmem_limit_bytes=67_043_328),
        )(x_rows.transpose(1, 0, 2), h_zero, c_zero, b_1, b_2.reshape(1, cols), w_x1, w_h1, w_x2, w_h2)
        return h_out[:, :batch], c_out[:, :batch]

    return jax.shard_map(local, mesh=mesh,
                         in_specs=(spec_seq, spec_weight, spec_weight, P(None, 'col'), spec_weight,
                                   P('row', 'col'), P('col'), spec_seq, spec_seq),
                         out_specs=(spec_out, spec_out), check_vma=False)
```

```python
import functools

import jax
import jax.numpy as jnp
from jax import lax
from jax.experimental import pallas as pl
from jax.experimental.pallas import tpu as pltpu
from jax.sharding import PartitionSpec as P

PAD = 8
STAGES = 4
BATCH = 2
FIRST_PIECE = 3
PIECES = 32
F32, BF16 = jnp.float32, jnp.bfloat16


def nbytes_wait(ref, sem):
    pltpu.make_async_copy(ref, ref, sem).wait()


def hop_groups(n_x, n_y):
    far = {}
    for dy in range(n_y):
        for dx in range(n_x):
            far.setdefault(min(dx, n_x - dx) + min(dy, n_y - dy), []).append((dx, dy))
    return [far[k] for k in sorted(far)]


def kernel(n_row, n_col, x_in, h_in, c_in, b1_in, b2_in, w_x1, w_h1, w_x2, w_h2, out_h, out_c,
           x_ref, h0_ref, c0_ref, bias, z_first, w_one, w_two, w_fwd, w_mid, send_a, send_c, stage, sort, p_b, p_f, xz_in, z_in, z_out, z_part, lhs,
           hs1, hs2, h_oth, c_all1, c_all2, c_st, ho, co,
           stage_sem, a_send, pass_sem, w_sem, f_send, f_sem, m_sem, c_send, c_sem, pf_send, pf_sem, pb_send, pb_sem, xz_send, xz_sem,
           mid_send, z_sem, init_send, h0_sem, c0_sem, step_send, step_sem, part_send, part_sem, row_sem,
           fwd_send, fwd_sem, end_send, end_sem):
    n_x = n_row // 2
    batch, n_step = x_in.shape[:2]
    n_bat = n_step // BATCH
    deep = w_h2.shape[0]
    wide = w_h2.shape[1] // n_row
    unit = wide // 4
    chunk = deep // 2
    r = lax.axis_index('row')
    y = lax.axis_index('col')
    core = lax.rem(r, 2)
    x = lax.div(r, 2)
    mate = r + 1 - 2 * core
    own_j = y * n_x + x

    def at(row, col):
        return {'row': row, 'col': col}

    def remote(src, dst, ssem, rsem, row, col):
        return pltpu.make_async_remote_copy(src_ref=src, dst_ref=dst, send_sem=ssem, recv_sem=rsem,
                                            device_id=at(row, col), device_id_type=pl.DeviceIdType.MESH)

    def group_of(i):
        near = jnp.logical_and(i >= 2, i < 6)
        dx = jnp.where(near, 1 + 2 * lax.rem(i, 2), jnp.where(i < 2, 2, 0))
        half = jnp.where(near, lax.div(i - 2, 2), lax.rem(i, 2))
        return lax.rem(x + dx, n_x), half

    def load(src, i, slot):
        tx, half = group_of(i)
        first = pl.multiple_of((2 * tx + half) * wide, wide)
        pltpu.make_async_copy(src.at[:, pl.ds(first, wide)], stage.at[slot], stage_sem.at[slot]).start()

    def load_late(n):
        slot, i = lax.rem(n, STAGES), lax.rem(n, n_row)

        @pl.when(n < n_row)
        def _():
            load(w_h2, i, slot)

        @pl.when(jnp.logical_and(n >= n_row, n < 3 * n_row))
        def _():
            load(w_x2.at[lax.div(n - n_row, n_row)], i, slot)

    def sorted_tile(slot):
        return jnp.dot(stage[slot], sort[...], preferred_element_type=F32).astype(BF16)

    def use_back(i, tile):
        tx, half = group_of(i)
        g = 2 * tx + half
        z_first[tx, half] = (jnp.dot(h0_ref[1, 0], tile[:chunk], preferred_element_type=F32)
                             + jnp.dot(h0_ref[1, 1], tile[chunk:], preferred_element_type=F32))

        @pl.when(jnp.logical_and(tx == x, core == 1))
        def _():
            w_one[r, half] = tile

        @pl.when(jnp.logical_or(tx != x, core == 0))
        def _():
            send_a[g] = tile

        @pl.when(jnp.logical_and(tx != x, core == 1))
        def _():
            remote(send_a.at[g], w_one.at[r, half], a_send, w_sem.at[0], 2 * tx + 1, y).start()

        @pl.when(jnp.logical_and(tx != x, core == 0))
        def _():
            remote(send_a.at[g], w_fwd.at[1, g], a_send, pass_sem.at[i], mate, y).start()

        @pl.when(jnp.logical_and(tx == x, core == 0))
        def _():
            remote(send_a.at[g], w_one.at[r, half], a_send, w_sem.at[0], mate, y).start()

    def pass_back(i, c):
        tx, half = group_of(i)
        g = 2 * tx + half
        nbytes_wait(w_fwd.at[1, g], pass_sem.at[i])
        remote(w_fwd.at[1, g], w_one.at[mate, half], a_send, w_sem.at[0], 2 * tx + 1, y).start()
        return c

    def use_fwd(i, tile):
        tx, half = group_of(i)
        g = 2 * tx + half
        w_fwd[0, g] = tile

        @pl.when(core == 1)
        def _():
            remote(w_fwd.at[0, g], w_fwd.at[1, g], f_send, f_sem, mate, y).start()

    def project(buf):
        def use(i, tile):
            tx, half = group_of(i)
            z = jnp.dot(x_ref[...], tile, preferred_element_type=F32)
            for m in range(n_bat):
                buf[m, tx, half] = z[m * BATCH * PAD:(m + 1) * BATCH * PAD]
        return use

    def late_tile(n):
        slot = lax.rem(n, STAGES)
        nbytes_wait(stage.at[slot], stage_sem.at[slot])
        load_late(n + STAGES - 1)
        tile = sorted_tile(slot)
        tx, half = group_of(lax.rem(n, n_row))
        g = 2 * tx + half

        @pl.when(n >= n_row)
        def _():
            k = lax.div(n - n_row, n_row)
            w_mid[k, g] = tile

            @pl.when(core == 1)
            def _():
                remote(w_mid.at[k, g], w_two.at[g, k], f_send, m_sem, mate, y).start()

        @pl.when(jnp.logical_and(n < n_row, jnp.logical_and(tx == x, core == 1)))
        def _():
            w_two[r, half] = tile

        @pl.when(jnp.logical_and(n < n_row, jnp.logical_or(tx != x, core == 0)))
        def _():
            send_c[g] = tile

        @pl.when(jnp.logical_and(n < n_row, jnp.logical_and(tx == x, core == 0)))
        def _():
            remote(send_c.at[g], w_two.at[r, half], c_send, w_sem.at[1], mate, y).start()

        @pl.when(jnp.logical_and(n < n_row, jnp.logical_and(tx != x, core == 1)))
        def _():
            remote(send_c.at[g], w_one.at[tx, half], c_send, c_sem, mate, y).start()

    def pieces(p):
        half, q = lax.div(p, 3 * PIECES), lax.rem(p, 3 * PIECES)
        k, e = lax.div(q, 3), lax.rem(q, 3)
        tx = lax.rem(x + jnp.where(e < 2, 1 + 2 * e, 2), n_x)
        n_rows = deep // PIECES
        rows = pl.ds(pl.multiple_of(k * n_rows, n_rows), n_rows)
        for src, owner in ((send_c.at[2 * tx + half, rows], r), (w_one.at[tx, half, rows], mate)):
            remote(src, w_two.at[owner, half, rows], c_send, w_sem.at[1], 2 * tx + 1, y).start()

    jobs = [(w_h1.at[1], use_back), (w_h1.at[0], use_fwd), (w_x1.at[0], project(p_f)), (w_x1.at[1], project(p_b))]
    for i in range(STAGES - 1):
        load(jobs[0][0], i, i)
    barrier = pltpu.get_barrier_semaphore()

    def greet():
        for dc in range(n_col):
            for dr in range(n_row):
                if dc or dr:
                    pl.semaphore_signal(barrier, inc=1, device_id=at(lax.rem(r + dr, n_row), lax.rem(y + dc, n_col)),
                                        device_id_type=pl.DeviceIdType.MESH)

    def iota2(shape):
        return lax.broadcasted_iota(jnp.int32, shape, 0), lax.broadcasted_iota(jnp.int32, shape, 1)

    def make_sort():
        rows_i, cols_i = iota2((wide, wide))
        gate_i, unit_i = lax.div(cols_i, unit), lax.rem(cols_i, unit)
        sort[...] = jnp.where(rows_i == 4 * unit_i + gate_i, 1.0, 0.0).astype(BF16)

    def pad_states():
        for k in range(3):
            lhs[0, 0:PAD, 0:deep] = jnp.zeros((PAD, deep), F32)
            lhs[0, 0:batch, 0:deep] = h_in[k]
            for jj in range(2):
                here = slice(jj * chunk, (jj + 1) * chunk)
                h0_ref[k, jj] = lhs[0, 0:PAD, here].astype(BF16)
                c0_ref[k, jj] = jnp.zeros((PAD, chunk), F32)
                c0_ref[k, jj, 0:batch] = c_in[k, :, here]

    greet()
    make_sort()
    pad_states()
    pl.semaphore_wait(barrier, n_col * n_row - 1)

    def share_states():
        for d in range(1, n_row):
            to = lax.rem(r + d, n_row)
            tc = lax.rem(to, 2)
            here = pl.ds(2 * r, 2)
            remote(h0_ref.at[tc], hs1.at[tc * n_step, here], init_send, h0_sem.at[0], to, y).start()
            remote(h0_ref.at[2], hs2.at[0, here], init_send, h0_sem.at[1], to, y).start()
            remote(c0_ref.at[tc], c_all1.at[here], init_send, c0_sem.at[0], to, y).start()
            remote(c0_ref.at[2], c_all2.at[here], init_send, c0_sem.at[1], to, y).start()
        hs1[core * n_step, pl.ds(2 * r, 2)] = h0_ref[core]
        hs2[0, pl.ds(2 * r, 2)] = h0_ref[2]
        c_all1[pl.ds(2 * r, 2)] = c0_ref[core]
        c_all2[pl.ds(2 * r, 2)] = c0_ref[2]

    share_states()

    def prepare():
        for hf in range(2):
            cols = pl.ds(pl.multiple_of((2 * x + hf) * wide, wide), wide)
            for n, b_row in enumerate((b1_in[pl.ds(core, 1), cols], b2_in[:, cols])):
                left = jnp.broadcast_to(b_row * 0.5, (PAD, wide))
                total = jnp.zeros((PAD, wide), F32)
                for _ in range(3):
                    part = left.astype(BF16)
                    total += jnp.dot(part, sort[...], preferred_element_type=F32)
                    left = left - part.astype(F32)
                bias[n, hf] = total * 2.0

        rows_i, cols_i = iota2((n_step * PAD, batch * n_step))
        take = jnp.where(cols_i == lax.rem(rows_i, PAD) * n_step + lax.div(rows_i, PAD), 1.0, 0.0)
        take = jnp.where(lax.rem(rows_i, PAD) < batch, take, 0.0).astype(BF16)
        flat = x_in[...].astype(F32).reshape(batch * n_step, deep).astype(BF16)
        x_ref[...] = jnp.dot(take, flat, preferred_element_type=F32).astype(BF16)

    for n, (src, use) in enumerate(jobs):
        def body(i, c):
            slot = lax.rem(i, STAGES)
            nbytes_wait(stage.at[slot], stage_sem.at[slot])
            ahead = i + STAGES - 1
            slot_ahead = lax.rem(ahead, STAGES)

            @pl.when(ahead < n_row)
            def _():
                load(src, ahead, slot_ahead)

            @pl.when(ahead >= n_row)
            def _():
                load(jobs[n + 1][0] if n + 1 < len(jobs) else w_h2, ahead - n_row, slot_ahead)
            use(i, sorted_tile(slot))
            return c
        lax.fori_loop(0, n_row, body, 0)
        if n == 0:
            @pl.when(core == 1)
            def _():
                lax.fori_loop(0, n_row - 2, pass_back, 0)
            prepare()
        if n == 2:
            @pl.when(core == 1)
            def _():
                remote(p_f, xz_in, pf_send, pf_sem, mate, y).start()

    p_b[n_bat - 1, :, :, (BATCH - 1) * PAD:] += z_first[...]

    nbytes_wait(hs1.at[0, pl.ds(0, 2 * n_row - 2)], h0_sem.at[0])
    nbytes_wait(hs2.at[0, pl.ds(0, 2 * n_row - 2)], h0_sem.at[1])
    nbytes_wait(c_all1.at[pl.ds(0, 2 * n_row - 2)], c0_sem.at[0])
    nbytes_wait(c_all2.at[pl.ds(0, 2 * n_row - 2)], c0_sem.at[1])

    def own_state(c_all):
        for hf in range(2):
            c_st[hf] = c_all[own_j, :, hf * unit:(hf + 1) * unit]
    own_state(c_all1)

    def rows_of(t):
        return pl.ds(pl.multiple_of(lax.rem(t, BATCH) * PAD, PAD), PAD)

    def cell(acc, hs, new):
        h_new = []
        for hf in range(2):
            gate = [acc[hf][:, k * unit:(k + 1) * unit] for k in range(4)]
            c = (jax.nn.sigmoid(gate[1]) * c_st[hf]
                 + jax.nn.sigmoid(gate[0]) * jnp.tanh(gate[2]))
            c_st[hf] = c
            h = (jax.nn.sigmoid(gate[3]) * jnp.tanh(c)).astype(BF16)
            hs[new, own_j, :, hf * unit:(hf + 1) * unit] = h
            h_new.append(h)
        return h_new

    def to_mate(slot):
        return remote(hs1.at[slot, pl.ds(x * n_x, n_x)], h_oth.at[slot], fwd_send, fwd_sem, mate, y)

    def mid(m, parts=(0, 1), after=False):
        for i in range(BATCH):
            for jj in range(n_x):
                here = slice(i * PAD, (i + 1) * PAD), slice(jj * chunk, (jj + 1) * chunk)
                if 0 in parts:
                    lhs[0, here[0], here[1]] = hs1[m * BATCH + i + 1, x * n_x + jj].astype(F32)
                if 1 in parts:
                    lhs[1, here[0], here[1]] = h_oth[m * BATCH + i, jj].astype(F32)
        left = {k: [lhs[k, :, c * deep:(c + 1) * deep].astype(BF16) for c in range(2)] for k in parts}

        def one(i, c):
            d = jnp.where(i == n_x - 1, 0, jnp.where(i == 0, 2, 2 * i - 1))
            tx = lax.rem(x + d, n_x)
            for hf in range(2):
                g = 2 * tx + hf
                z = p_b[m, tx, hf] if after else jnp.zeros((BATCH * PAD, wide), F32)
                for k in parts:
                    z += jnp.dot(left[k][0], w_mid[k, g], preferred_element_type=F32)
                    z += jnp.dot(left[k][1], w_two[g, k], preferred_element_type=F32)
                p_b[m, tx, hf] = z
            if 1 in parts:
                remote(p_b.at[m, tx], z_in.at[m, lax.rem(n_x - d, n_x)], mid_send, z_sem.at[m], 2 * tx + 1, y).start()
            return c
        lax.fori_loop(0, n_x, one, 0)

    sends = [o for grp in hop_groups(n_x, n_col) for o in grp][:0:-1]

    def along(pos, n):
        inner = lax.rem(1 - 2 * lax.rem(pos, 2) + n, n)
        return {'0': 0, 'I': inner, 'O': n - inner, 'F': n // 2}
    dxs, dys = along(x, n_x), along(y, n_col)
    groups = [g.split() for g in ('00', 'I0', '0I', 'II', 'O0 0O', 'F0 0F', 'IO OI OO', 'FI IF', 'FO OF FF')]

    def source(name):
        dx, dy = dxs[name[0]], dys[name[1]]
        return lax.rem(y + dy, n_col) * n_x + lax.rem(x + dx, n_x), dy * n_x + dx

    def chain_step(hs, w, prev, new, s, z_of, layer, first, last_send, after_receive):
        parity = lax.rem(s, 2)
        acc = [bias[layer, hf] if first else z_of(hf) + bias[layer, hf] for hf in range(2)]
        for n, grp in enumerate(groups):
            if first and layer == 0:
                break
            if n and not first:
                for name in grp:
                    j, i = source(name)
                    nbytes_wait(hs.at[prev, j], step_sem.at[1 - parity, i])
            if n == len(groups) - 1 and not first:
                after_receive()
            for name in grp:
                j, _ = source(name)
                h = hs[prev, j]
                rows = pl.ds(pl.multiple_of(lax.rem(j, 2) * chunk, chunk), chunk)
                for hf in range(2):
                    acc[hf] += jnp.dot(h, w[lax.div(j, 2), hf, rows], preferred_element_type=F32)
        if first:
            acc = [acc[hf] + z_of(hf) for hf in range(2)]
        h_new = cell(acc, hs, new)

        def send():
            for dx, dy in sends:
                remote(hs.at[new, own_j], hs.at[new, own_j], step_send,
                       step_sem.at[parity, (n_col - dy) % n_col * n_x + (n_x - dx) % n_x],
                       2 * lax.rem(x + dx, n_x) + 1, lax.rem(y + dy, n_col)).start()
        if last_send:
            send()
        else:
            pl.when(s < n_step - 1)(send)
        return h_new

    @pl.when(core == 1)
    def _():
        for m in reversed(range(n_bat)):
            remote(p_b.at[m], z_in.at[m], pb_send, pb_sem.at[m], mate, y).start()

        def tiles(n, c):
            late_tile(n)
            return c
        lax.fori_loop(0, 3 * n_row, tiles, 0)

        def step_one(s, c, first=False):
            t = n_step - 1 - s
            m, rows = lax.div(t, BATCH), rows_of(t)

            if not first:
                @pl.when(lax.rem(s, BATCH) == 0)
                def _():
                    nbytes_wait(xz_in.at[m], xz_sem.at[m])

            def z_of(hf):
                if first and hf == 0:
                    nbytes_wait(xz_in.at[m], xz_sem.at[m])
                z = xz_in[m, 0, hf, rows]
                for d in range(1, n_x):
                    z = z + xz_in[m, d, hf, rows]
                return z

            chain_step(hs1, w_one, t + 1, t, s, z_of, 0, first, True, lambda: to_mate(t + 1).start())
            return c
        step_one(jnp.int32(0), 0, True)
        nbytes_wait(w_one.at[pl.ds(0, n_row - 1)], w_sem.at[0])
        lax.fori_loop(1, n_step, step_one, 0)
        for grp in groups[1:]:
            for name in grp:
                j, i = source(name)
                nbytes_wait(hs1.at[0, j], step_sem.at[(n_step - 1) % 2, i])
        to_mate(0).start()
        co[1] = c_st[0]
        out_c[1] = c_st[1]
        own_state(c_all2)
        nbytes_wait(w_two.at[pl.ds(0, n_row - 1)], w_sem.at[1])

        def step_two(t, c, first=False):
            m, rows = lax.div(t, BATCH), rows_of(t)

            if not first:
                @pl.when(lax.rem(t, BATCH) == 0)
                def _():
                    nbytes_wait(z_in.at[m], z_sem.at[m])

            def z_of(hf):
                if first and hf == 0:
                    nbytes_wait(z_in.at[m], z_sem.at[m])
                z = z_in[m, 0, hf, rows]
                for d in range(1, n_x):
                    z = z + z_in[m, d, hf, rows]
                return z
            h_new = chain_step(hs2, w_two, t, t + 1, t, z_of, 1, first, False, lambda: None)
            ho[t] = h_new[0]
            out_h[t] = h_new[1]
            return c
        step_two(jnp.int32(0), 0, True)
        lax.fori_loop(1, n_step, step_two, 0)
        co[2] = c_st[0]
        out_c[2] = c_st[1]
        ends = [remote(ho, out_h, end_send.at[0], end_sem.at[0], mate, y),
                remote(co.at[pl.ds(1, 2)], out_c.at[pl.ds(1, 2)], end_send.at[1], end_sem.at[1], mate, y)]
        for e in ends:
            e.start()
        for e in ends:
            e.wait_send()
        nbytes_wait(out_c.at[0], end_sem.at[2])
        nbytes_wait(hs1.at[pl.ds(0, n_step), pl.ds(0, n_x * n_col - 1)], step_send)
        nbytes_wait(hs2.at[pl.ds(0, n_step - 1), pl.ds(0, n_x * n_col - 1)], step_send)
        nbytes_wait(p_b, pb_send)
        nbytes_wait(h_oth, fwd_send)
        nbytes_wait(p_f, pf_send)
        nbytes_wait(w_fwd.at[0], f_send)
        nbytes_wait(w_mid, f_send)
        nbytes_wait(send_a.at[pl.ds(0, n_row - 2)], a_send)
        nbytes_wait(send_a.at[pl.ds(0, n_row - 2)], a_send)
        nbytes_wait(send_c.at[pl.ds(0, n_row - 2)], c_send)

    @pl.when(core == 0)
    def _():
        def send_batch(m):
            nbytes_wait(z_in.at[m], pb_sem.at[m])
            for d in (2, 1, 3, 0):
                tx = lax.rem(x + d, n_x)
                p_b[m, tx] += z_in[m, tx]
                remote(p_b.at[m, tx], xz_in.at[m, (n_x - d) % n_x], xz_send, xz_sem.at[m], 2 * tx + 1, y).start()
        send_batch(n_bat - 1)
        send_batch(n_bat - 2)
        nbytes_wait(xz_in, pf_sem)
        nbytes_wait(w_fwd.at[1], f_sem)
        first_mid = n_step - 11

        def receive_rows(slot, parity):
            for k in range(n_x):
                @pl.when(jnp.logical_or(x != k, x != y))
                def _():
                    nbytes_wait(hs1.at[slot, x * n_x + k], row_sem.at[parity, k])

        def step_fwd(t, c):
            m, rows, parity = lax.div(t, BATCH), rows_of(t), lax.rem(t, 2)

            @pl.when(t > 0)
            def _():
                receive_rows(t, 1 - parity)
            hv = [hs1[t, x * n_x + k] for k in range(n_x)]
            for d in (1, 3, 2, 0):
                tx = lax.rem(x + d, n_x)
                for hf in range(2):
                    acc = p_f[m, tx, hf, rows] + xz_in[m, tx, hf, rows]
                    for k in range(n_x):
                        acc += jnp.dot(hv[k], w_fwd[k // 2, 2 * tx + hf, (k % 2) * chunk:(k % 2 + 1) * chunk],
                                       preferred_element_type=F32)
                    z_out[parity, tx, hf] = acc
                if d:
                    remote(z_out.at[parity, tx], z_part.at[parity, n_x - 1 - d], part_send,
                           part_sem.at[parity, n_x - 1 - d], 2 * tx, y).start()

            def share(k):
                @pl.when(t < 3 * n_row // 4)
                def _():
                    late_tile(4 * t + 2 * k)
                    late_tile(4 * t + 2 * k + 1)

                for p in range(12 - 4 * k):
                    nth = 20 * (t - FIRST_PIECE) + 12 * k + p

                    @pl.when(jnp.logical_and(t >= FIRST_PIECE, nth < 6 * PIECES))
                    def _():
                        pieces(nth)

            @pl.when(t == FIRST_PIECE)
            def _():
                nbytes_wait(w_one.at[pl.ds(0, n_x - 1)], c_sem)
            share(0)

            @pl.when(t == first_mid)
            def _():
                nbytes_wait(p_b, xz_send)
                nbytes_wait(w_two, m_sem)
                mid(0, (0,))
                nbytes_wait(h_oth, fwd_sem)
                mid(0, (1,), True)

            @pl.when(jnp.logical_and(t > first_mid, jnp.logical_or(t < first_mid + 4, jnp.logical_and(t > first_mid + 4, lax.rem(t, 2) == 0))))
            def _():
                mid(jnp.where(t < first_mid + 4, 2 * (t - first_mid), lax.div(t, 2) - 1))

            for d in range(n_x - 1):
                nbytes_wait(z_part.at[parity, d], part_sem.at[parity, d])
            acc = []
            for hf in range(2):
                z = z_out[parity, x, hf] + bias[0, hf]
                for d in range(n_x - 1):
                    z = z + z_part[parity, d, hf]
                acc.append(z)
            cell(acc, hs1, t + 1)
            for k in range(n_col):
                to_y = lax.rem(y + k, n_col)

                def give():
                    remote(hs1.at[t + 1, own_j], hs1.at[t + 1, own_j], step_send, row_sem.at[parity, x],
                           2 * y, to_y).start()
                if k:
                    give()
                else:
                    pl.when(x != y)(give)

            share(1)

            @pl.when(jnp.logical_and(t >= 1, t < n_bat - 1))
            def _():
                send_batch(n_bat - 2 - t)

            @pl.when(jnp.logical_and(t >= first_mid, t < first_mid + 4))
            def _():
                mid(2 * (t - first_mid) + 1)
            nbytes_wait(z_out.at[0, pl.ds(0, n_x - 1)], part_send)
            return c
        lax.fori_loop(0, n_step, step_fwd, 0)
        receive_rows(n_step, (n_step - 1) % 2)
        mid(n_bat - 1)
        out_c[0] = c_st[0]
        co[0] = c_st[1]
        e = remote(co.at[0], out_c.at[0], end_send.at[2], end_sem.at[2], mate, y)
        e.start()
        e.wait_send()
        nbytes_wait(out_h, end_sem.at[0])
        nbytes_wait(out_c.at[pl.ds(1, 2)], end_sem.at[1])
        nbytes_wait(p_b, mid_send)
        nbytes_wait(send_a, a_send)
        nbytes_wait(send_c, c_send)
        nbytes_wait(send_c.at[pl.ds(0, n_row - 2)], c_send)
        nbytes_wait(hs1.at[pl.ds(0, n_step), pl.ds(0, n_col - 1)], step_send)

        @pl.when(x != y)
        def _():
            nbytes_wait(hs1.at[pl.ds(0, n_step), 0], step_send)

    nbytes_wait(hs1.at[0, pl.ds(0, 2 * n_row - 2)], init_send)
    nbytes_wait(hs1.at[0, pl.ds(0, 2 * n_row - 2)], init_send)
    nbytes_wait(c_all1.at[pl.ds(0, 2 * n_row - 2)], init_send)
    nbytes_wait(c_all1.at[pl.ds(0, 2 * n_row - 2)], init_send)


def solution(mesh):
    n_row = mesh.shape['row']
    n_col = mesh.shape['col']
    spec_seq = P(None, 'data', 'row')
    spec_weight = P(None, 'row', 'col')
    spec_out = P(None, 'data', ('col', 'row'))

    def local(x_rows, w_x1, w_h1, b_1, w_x2, w_h2, b_2, h_zero, c_zero):
        n_step, batch, deep = x_rows.shape
        cols = w_h2.shape[1]
        wide = cols // n_row
        unit = wide // 4
        n_chunk = n_row // 2 * n_col
        chunk = 2 * unit
        n_bat = n_step // BATCH
        n_x = n_row // 2

        vmem = pl.BlockSpec(memory_space=pltpu.VMEM)
        hbm = pl.BlockSpec(memory_space=pl.ANY)
        dma = pltpu.SemaphoreType.DMA
        rows = BATCH * PAD
        weights = (n_row, 2, deep, wide)
        h_out, c_out = pl.pallas_call(
            functools.partial(kernel, n_row, n_col),
            out_shape=(jax.ShapeDtypeStruct((n_step, PAD, unit), BF16),
                       jax.ShapeDtypeStruct((3, PAD, unit), F32)),
            in_specs=[vmem] * 5 + [hbm] * 4,
            out_specs=(vmem, vmem),
            scratch_shapes=[
                pltpu.VMEM((n_step * PAD, deep), BF16),
                pltpu.VMEM((3, 2, PAD, chunk), BF16),
                pltpu.VMEM((3, 2, PAD, chunk), F32),
                pltpu.VMEM((2, 2, PAD, wide), F32),
                pltpu.VMEM((n_x, 2, PAD, wide), F32),
                pltpu.VMEM(weights, BF16),
                pltpu.VMEM(weights, BF16),
                pltpu.VMEM((2, n_row, deep, wide), BF16),
                pltpu.VMEM((2, n_row, deep, wide), BF16),
                pltpu.VMEM((n_row, deep, wide), BF16),
                pltpu.VMEM((n_row, deep, wide), BF16),
                pltpu.VMEM((STAGES, deep, wide), BF16),
                pltpu.VMEM((wide, wide), BF16),
                pltpu.VMEM((n_bat, n_x, 2, rows, wide), F32),
                pltpu.VMEM((n_bat, n_x, 2, rows, wide), F32),
                pltpu.VMEM((n_bat, n_x, 2, rows, wide), F32),
                pltpu.VMEM((n_bat, n_x, 2, rows, wide), F32),
                pltpu.VMEM((2, n_x, 2, PAD, wide), F32),
                pltpu.VMEM((2, n_x - 1, 2, PAD, wide), F32),
                pltpu.VMEM((2, rows, 2 * deep), F32),
                pltpu.VMEM((n_step + 1, n_chunk, PAD, chunk), BF16),
                pltpu.VMEM((n_step + 1, n_chunk, PAD, chunk), BF16),
                pltpu.VMEM((n_step, n_x, PAD, chunk), BF16),
                pltpu.VMEM((n_chunk, PAD, chunk), F32),
                pltpu.VMEM((n_chunk, PAD, chunk), F32),
                pltpu.VMEM((2, PAD, unit), F32),
                pltpu.VMEM((n_step, PAD, unit), BF16),
                pltpu.VMEM((3, PAD, unit), F32),
                dma((STAGES,)), dma(()), dma((n_row,)), dma((2,)),
                dma(()), dma(()), dma(()), dma(()), dma(()),
                dma(()), dma(()), dma(()), dma((n_bat,)),
                dma(()), dma((n_bat,)), dma(()), dma((n_bat,)),
                dma(()), dma((2,)), dma((2,)),
                dma(()), dma((2, n_chunk)),
                dma(()), dma((2, n_x - 1)), dma((2, n_x)),
                dma(()), dma(()),
                dma((3,)), dma((3,)),
            ],
            compiler_params=pltpu.CompilerParams(collective_id=0, has_side_effects=True,
                                                 vmem_limit_bytes=67_043_328),
        )(x_rows.transpose(1, 0, 2), h_zero, c_zero, b_1, b_2.reshape(1, cols), w_x1, w_h1, w_x2, w_h2)
        return h_out[:, :batch], c_out[:, :batch]

    return jax.shard_map(local, mesh=mesh,
                         in_specs=(spec_seq, spec_weight, spec_weight, P(None, 'col'), spec_weight,
                                   P('row', 'col'), P('col'), spec_seq, spec_seq),
                         out_specs=(spec_out, spec_out), check_vma=False)
```
